256 devices in a mesh: dp: 64 (over y, z, core), outer: 4 (over x).
Axes of the slice: x: 4, y: 4, z: 8, core: 2. Of those that a mesh axis runs over, the one named last changes fastest.
Arguments:
- clean: bfloat16 [2048, 112, 1024], P(('dp', 'outer')), may hold values from -3 to 3
- noise: bfloat16 [2048, 112, 1024], P(('dp', 'outer')), may hold values from -6 to 6
- t_index: int32 [2048], P(('dp', 'outer')), may hold values from 0 to 1278
- bucket_id: int32 [2048], P(('dp', 'outer')), may hold values from 0 to 15
- bucket_count: int32 [16], replicated, may hold values from 1 to 999
- w_first: bfloat16 [1024, 1024], replicated, may hold values from -0.5 to 0.5
- w_second: bfloat16 [1024, 1024], replicated, may hold values from -0.5 to 0.5
- teacher_first: bfloat16 [1024, 1024], replicated, may hold values from -0.5 to 0.5
- teacher_second: bfloat16 [1024, 1024], replicated, may hold values from -0.5 to 0.5
Outputs:
- grad_first: float32 [1024, 1024], P(('dp', 'outer'))
- grad_second: float32 [1024, 1024], P(('dp', 'outer'))
- bucket_loss: float32 [16], replicated
The draws below stay inside these ranges and needn't reach their ends.
All inputs are finite; a program needn't handle non-finite values.
Results may differ from the reference program's by a relative error of at most 0.0033.
Values sent between devices are 32-bit elements; how exact they have to be, the bound alone decides.
No kernel may reach another device: no remote copies, remote signals or barrier semaphores. Data moves between devices by JAX's collectives and lax.ppermute only.
A program may use at most 128 MiB of HBM per device.

```python
import math
import jax
import jax.numpy as jnp
from jax import lax

D = 1024
H = 1024
PATCHES = 112
LAT_DEV = 8
STEPS = 1280
BUCKETS = 16
LATENTS = 2048


drift_scale = 0.3


def weight_pair(key, fan_in, rows, cols, salt):
    pair_key = jax.random.fold_in(key, salt)
    base_key = jax.random.fold_in(pair_key, 1)
    drift_key = jax.random.fold_in(pair_key, 2)
    spread = 1.0 / math.sqrt(fan_in)
    base = jax.random.truncated_normal(base_key, -6.0, 6.0, (rows, cols), jnp.float32) * spread
    drift = jax.random.truncated_normal(drift_key, -6.0, 6.0, (rows, cols), jnp.float32) * (drift_scale * spread)
    return (base, base + drift)


def draw_w_first(key, part):
    return weight_pair(key, D, D, H, 11)[0].astype(jnp.bfloat16)


def draw_teacher_first(key, part):
    return weight_pair(key, D, D, H, 11)[1].astype(jnp.bfloat16)


def draw_w_second(key, part):
    return weight_pair(key, H, H, D, 12)[0].astype(jnp.bfloat16)


def draw_teacher_second(key, part):
    return weight_pair(key, H, H, D, 12)[1].astype(jnp.bfloat16)


def with_ends(array, stream_key, smallest, largest):
    index_at = [jax.random.randint(jax.random.fold_in(stream_key, axis), (), 0, length) for axis, length in enumerate(array.shape)]
    widest = array.shape.index(max(array.shape))
    neighbour = index_at[:widest] + [(index_at[widest] + 1) % array.shape[widest]] + index_at[widest + 1:]
    return array.at[tuple(index_at)].set(smallest).at[tuple(neighbour)].set(largest)


def steps_of(rng, extent, split, low, largest):
    def one(position, shards_of):
        heights = jax.random.uniform(jax.random.fold_in(jax.random.fold_in(rng, 6), position), (shards_of,), jnp.float32, low / len(split), largest / len(split))
        return jnp.repeat(jnp.exp(heights), extent[position] // shards_of).reshape((-1,) + (1,) * (len(extent) - position - 1))

    loudness = one(*split[0])
    for cut in split[1:]:
        loudness = loudness * one(*cut)
    return loudness


def gaussian(key, extent, scale, most, split=(), kind=jnp.bfloat16):
    drawn = scale * jax.random.normal(key, extent, jnp.float32)
    if split:
        drawn = drawn * steps_of(key, extent, split, -0.22, 0.18)
    return jnp.clip(drawn, -most, most).astype(kind)


def setup_inputs(seed: int = 0) -> dict:
    splits = jax.random.split(jax.random.key(seed), 10)
    clean = gaussian(splits[0], (LATENTS, PATCHES, D), 0.5, 3.0, ((0, 256),))
    noise = gaussian(splits[1], (LATENTS, PATCHES, D), 1.0, 6.0, ((0, 256),))
    t_index = with_ends(jax.random.randint(splits[2], (LATENTS,), 0, STEPS - 1), jax.random.fold_in(splits[2], 1), 0, (STEPS - 1) - 1).astype(jnp.int32)
    bucket_id = with_ends(jax.random.randint(splits[3], (LATENTS,), 0, BUCKETS), jax.random.fold_in(splits[3], 1), 0, BUCKETS - 1).astype(jnp.int32)
    bucket_count = with_ends(jax.random.randint(splits[4], (BUCKETS,), 1, 1000), jax.random.fold_in(splits[4], 1), 1, 999).astype(jnp.int32)
    w_first = draw_w_first(jax.random.fold_in(splits[9], 71), 0)
    w_second = draw_w_second(jax.random.fold_in(splits[9], 71), 0)
    teacher_first = draw_teacher_first(jax.random.fold_in(splits[9], 71), 0)
    teacher_second = draw_teacher_second(jax.random.fold_in(splits[9], 71), 0)
    return {"clean": clean, "noise": noise, "t_index": t_index, "bucket_id": bucket_id, "bucket_count": bucket_count, "w_first": w_first, "w_second": w_second, "teacher_first": teacher_first, "teacher_second": teacher_second}


sigma_floor = 0.002
sigma_ceiling = 80.0
sigma_data = 0.5
huber_scale = 0.00054
rho_power = 7.0

def plan(index):
    ramp = index.astype(jnp.float32) / (STEPS - 1)
    top = sigma_ceiling ** (1.0 / rho_power)
    bottom = sigma_floor ** (1.0 / rho_power)
    return (top + ramp * (bottom - top)) ** rho_power

def scale_factors(noise_level):
    skip_scale = sigma_data ** 2 / ((noise_level - sigma_floor) ** 2 + sigma_data ** 2)
    outer_scale_factor = (noise_level - sigma_floor) * sigma_data / jnp.sqrt(noise_level ** 2 + sigma_data ** 2)
    inner_product = 1.0 / jnp.sqrt(noise_level ** 2 + sigma_data ** 2)
    return (skip_scale, outer_scale_factor, inner_product)

def network(field, noise_level_rows, first, second):
    skip_scale, outer_scale_factor, inner_product = scale_factors(noise_level_rows)
    inputs = (inner_product * field).astype(jnp.bfloat16)
    pre = jnp.dot(inputs, first, preferred_element_type=jnp.float32)
    active = jax.nn.silu(pre).astype(jnp.bfloat16)
    result = skip_scale * field + outer_scale_factor * jnp.dot(active, second, preferred_element_type=jnp.float32)
    return (result, inputs, pre, active, outer_scale_factor)

def block_terms(clean, noise, t_index, bucket_id, bucket_count, w_first, w_second, teacher_first, teacher_second, total):
    latents, patches, width = clean.shape
    rows = latents * patches
    sig_hi = plan(t_index)
    sig_lo = plan(t_index + 1)
    clean_f = clean.astype(jnp.float32)
    noise_f = noise.astype(jnp.float32)
    x_hi = (clean_f + sig_hi[:, None, None] * noise_f).reshape(rows, width)
    x_lo = (clean_f + sig_lo[:, None, None] * noise_f).reshape(rows, width)
    rows_hi = jnp.repeat(sig_hi, patches)[:, None]
    rows_lo = jnp.repeat(sig_lo, patches)[:, None]
    online, inputs, pre, active, outer_scale_factor = network(x_hi, rows_hi, w_first, w_second)
    target = network(x_lo, rows_lo, teacher_first, teacher_second)[0]
    diff = (online - target).reshape(latents, patches * width)
    sumsq = lax.optimization_barrier(jnp.sum(diff * diff, axis=1))
    huber_c = huber_scale * math.sqrt(patches * width)
    root = jnp.sqrt(sumsq + huber_c ** 2)
    distance = root - huber_c
    onehot = (bucket_id[:, None] == jnp.arange(bucket_count.shape[0], dtype=jnp.int32)[None, :]).astype(jnp.float32)
    count_each = lax.optimization_barrier(jnp.sum(onehot * bucket_count.astype(jnp.float32)[None, :], axis=1))
    weight = sig_lo / (sig_hi - sig_lo) / jnp.sqrt(count_each) / total
    bucket_part = lax.optimization_barrier(jnp.sum(onehot * (weight * distance)[:, None], axis=0))
    coef = weight / root
    grad_out = ((coef[:, None] * diff).reshape(rows, width) * outer_scale_factor).astype(jnp.bfloat16)
    grad_second = jnp.dot(active.T, grad_out, preferred_element_type=jnp.float32)
    grad_active = jnp.dot(grad_out, w_second.T, preferred_element_type=jnp.float32)
    gate = jax.nn.sigmoid(pre)
    grad_pre = (grad_active * gate * (1.0 + pre * (1.0 - gate))).astype(jnp.bfloat16)
    grad_first = jnp.dot(inputs.T, grad_pre, preferred_element_type=jnp.float32)
    return (grad_first, grad_second, bucket_part)

def reference(clean, noise, t_index, bucket_id, bucket_count, w_first, w_second, teacher_first, teacher_second):
    blocks = LATENTS // LAT_DEV
    clean_batch = clean.reshape(blocks, LAT_DEV, PATCHES, D)
    noise_b = noise.reshape(blocks, LAT_DEV, PATCHES, D)
    index_b = t_index.reshape(blocks, LAT_DEV)
    bucket_b = bucket_id.reshape(blocks, LAT_DEV)

    def step(carry, items):
        first, second, part = block_terms(items[0], items[1], items[2], items[3], bucket_count, w_first, w_second, teacher_first, teacher_second, LATENTS)
        return ((carry[0] + first, carry[1] + second, carry[2] + part), None)
    start = (jnp.zeros((D, H), jnp.float32), jnp.zeros((H, D), jnp.float32), jnp.zeros((BUCKETS,), jnp.float32))
    totals = lax.scan(step, start, (clean_batch, noise_b, index_b, bucket_b))[0]
    return (totals[0], totals[1], totals[2])
```

```python
import functools, math
import jax, jax.numpy as jnp
from jax import lax
from jax.experimental import pallas as pl
from jax.experimental.pallas import tpu as pltpu
from jax.sharding import Mesh
from jax.sharding import PartitionSpec as P

DP_OUTER = ("dp_0", "dp_1", "dp_2", "outer")

STEPS = 1280
sigma_floor = 0.002
sigma_ceiling = 80.0
sigma_data = 0.5
huber_scale = 0.00054
rho_power = 7.0
F32, BF16 = jnp.float32, jnp.bfloat16
PATCHES, D, H = 112, 1024, 1024
TILE = (8, 128)
TN = 256
LAT = 8
VMEM = pl.BlockSpec(memory_space=pltpu.VMEM)
SMEM = pl.BlockSpec(memory_space=pltpu.SMEM)
ANY = pl.BlockSpec(memory_space=pl.ANY)


def rows_from(values):
    row = lax.broadcasted_iota(jnp.int32, TILE, 0)
    out = jnp.full(TILE, values[0])
    for k in range(1, len(values)):
        out = jnp.where(row == k, values[k], out)
    return out


def plan(index):
    ramp = index.astype(F32) / (STEPS - 1)
    top = sigma_ceiling ** (1.0 / rho_power)
    bottom = sigma_floor ** (1.0 / rho_power)
    base = top + ramp * (bottom - top)
    square = base * base
    fourth = square * square
    return fourth * square * base


def scale_factors(s):
    skip = sigma_data**2 / ((s - sigma_floor) ** 2 + sigma_data**2)
    scale = jnp.sqrt(s * s + sigma_data**2)
    return skip, (s - sigma_floor) * sigma_data / scale, 1.0 / scale


def store_routed(block, y, t, core, keep_ref, send_ref):
    v = block.reshape(32, 8, 256)
    left, right = v[:, :, :128], v[:, :, 128:]
    halves = (
        jnp.concatenate([left[:, :4], right[:, :4]], axis=1),
        jnp.concatenate([left[:, 4:], right[:, 4:]], axis=1),
    )
    for x in range(4):
        pieces = halves[x % 2].reshape(8, 2, 2, 8, 128)[:, :, x // 2]
        c0, c1 = pieces[:, 0], pieces[:, 1]
        if t < 2:
            at = ((x * 4 + y) * 2 + t) * 8
        else:
            at = 256 + ((y * 4 + x) * 2 + t - 2) * 8
        keep_ref[pl.ds(at, 8)] = jnp.where(core == 0, c0, c1)
        send_ref[pl.ds(at, 8)] = jnp.where(core == 0, c1, c0)


def forward_kernel(place, t_index, bucket_id, bucket_count, clean, noise, w1, w2, t1, t2,
                   keep, send, grad_out, gate, inputs,
                   in_lo, act_hi, act_lo, diff, coef, wbuf, sems, *, total, MB):
    copies = [pltpu.make_async_copy(src, wbuf.at[k], sems.at[k]) for k, src in enumerate((w1, t1, w2, t2))]
    for copy in copies:
        copy.start()
    hi_index = rows_from([t_index[k] for k in range(LAT)])
    s_hi, s_lo = plan(hi_index), plan(hi_index + 1)
    skip_hi, out_hi, in_scale_hi = scale_factors(s_hi)
    skip_lo, out_lo, in_scale_lo = scale_factors(s_lo)
    coef[0] = s_hi
    coef[1] = s_lo
    coef[2] = in_scale_hi
    coef[3] = in_scale_lo
    coef[4] = skip_hi
    coef[5] = skip_lo
    coef[6] = out_hi
    coef[7] = out_lo

    def one(k, lat):
        return coef[k, pl.ds(lat, 1), 0:1]

    def field(lat, _):
        rows = pl.ds(lat * PATCHES, PATCHES)
        c, n = clean[rows, :].astype(F32), noise[rows, :].astype(F32)
        inputs[rows, :] = (one(2, lat) * (c + one(0, lat) * n)).astype(BF16)
        in_lo[rows, :] = (one(3, lat) * (c + one(1, lat) * n)).astype(BF16)
        return 0
    lax.fori_loop(0, LAT, field, 0)
    copies[0].wait()
    copies[1].wait()
    NB = 896 // MB

    def hidden(i, _):
        rows = pl.ds(pl.multiple_of((i % NB) * MB, MB), MB)
        cols = pl.ds(pl.multiple_of((i // NB) * TN, TN), TN)
        pre = jnp.dot(inputs[rows, :], wbuf[0, :, cols], preferred_element_type=F32)
        sig = jax.nn.sigmoid(pre)
        act_hi[rows, cols] = (pre * sig).astype(BF16)
        gate[rows, cols] = sig * (1.0 + pre * (1.0 - sig))
        pre = jnp.dot(in_lo[rows, :], wbuf[1, :, cols], preferred_element_type=F32)
        act_lo[rows, cols] = (pre * jax.nn.sigmoid(pre)).astype(BF16)
        return 0
    lax.fori_loop(0, NB * 4, hidden, 0)
    copies[2].wait()
    copies[3].wait()

    def outer(i, sums):
        first = (i % NB) * MB
        rows = pl.ds(pl.multiple_of(first, MB), MB)
        cols = pl.ds(pl.multiple_of((i // NB) * TN, TN), TN)
        online = jnp.dot(act_hi[rows, :], wbuf[2, :, cols], preferred_element_type=F32)
        target = jnp.dot(act_lo[rows, :], wbuf[3, :, cols], preferred_element_type=F32)
        row = lax.broadcasted_iota(jnp.int32, TILE, 0)
        for k in range(MB // PATCHES):
            lat = (i % NB) * (MB // PATCHES) + k
            r = pl.ds(lat * PATCHES, PATCHES)
            s = slice(k * PATCHES, (k + 1) * PATCHES)
            c, n = clean[r, cols].astype(F32), noise[r, cols].astype(F32)
            on = one(4, lat) * (c + one(0, lat) * n) + one(6, lat) * online[s]
            tg = one(5, lat) * (c + one(1, lat) * n) + one(7, lat) * target[s]
            d = on - tg
            diff[r, cols] = d
            sq = jnp.sum((d * d).reshape(PATCHES // 8, 8, TN // 128, 128), axis=(0, 2))
            sums = sums + jnp.where(row == lat, jnp.sum(sq, axis=0, keepdims=True), 0.0)
        return sums
    sums = lax.fori_loop(0, NB * 4, outer, jnp.zeros(TILE, F32))
    q = jnp.sum(sums, axis=1, keepdims=True)
    c2 = huber_scale * math.sqrt(PATCHES * D)
    root = jnp.sqrt(q + c2**2)
    distance = root - c2
    count = rows_from([bucket_count[bucket_id[k]].astype(F32) for k in range(LAT)])
    weight = s_lo / (s_hi - s_lo) / jnp.sqrt(count) / total
    lane = lax.broadcasted_iota(jnp.int32, TILE, 1)
    bucket = jnp.where(lane == rows_from([bucket_id[k] for k in range(LAT)]), weight * distance, 0.0)
    keep[512] = bucket
    send[512] = bucket
    coef[0] = weight / root

    def grad(lat, _):
        rows = pl.ds(lat * PATCHES, PATCHES)
        grad_out[rows, :] = (one(0, lat) * diff[rows, :] * one(6, lat)).astype(BF16)
        return 0
    lax.fori_loop(0, LAT, grad, 0)
    core = place[0]

    for t in range(4):
        def second(y, _):
            block = lax.dot_general(act_hi[:, pl.ds(pl.multiple_of(y * 256, 256), 256)], grad_out[:, t * 256:(t + 1) * 256],
                                    (((0,), (0,)), ((), ())), preferred_element_type=F32)
            store_routed(block, y, t, core, keep, send)
            return 0
        lax.fori_loop(0, 4, second, 0)


def first_kernel(place, grad_out, gate, inputs, w2, keep, send, grad_pre):
    core = place[0]
    for t in range(4):
        cols = slice(t * 256, (t + 1) * 256)
        for m in range(2):
            rows = slice(m * 448, (m + 1) * 448)
            back = lax.dot_general(grad_out[rows, :], w2[cols, :], (((1,), (1,)), ((), ())), preferred_element_type=F32)
            grad_pre[rows, :] = (back * gate[rows, cols]).astype(BF16)

        def first(y, _):
            block = lax.dot_general(inputs[:, pl.ds(pl.multiple_of(y * 256, 256), 256)], grad_pre[...],
                                    (((0,), (0,)), ((), ())), preferred_element_type=F32)
            store_routed(block, y, t, core, keep, send)
            return 0
        lax.fori_loop(0, 4, first, 0)


def tiles(n):
    return jax.ShapeDtypeStruct((n, 8, 128), F32)


def forward(place, t_index, bucket_id, bucket_count, clean, noise, w1, w2, t1, t2, total, MB=448):
    rows = 896
    return pl.pallas_call(
        functools.partial(forward_kernel, total=total, MB=MB),
        out_shape=(tiles(513), tiles(513), jax.ShapeDtypeStruct((rows, D), BF16),
                   jax.ShapeDtypeStruct((rows, H), F32), jax.ShapeDtypeStruct((rows, D), BF16)),
        in_specs=[SMEM] * 4 + [VMEM] * 2 + [ANY] * 4,
        out_specs=(VMEM,) * 5,
        scratch_shapes=[pltpu.VMEM((rows, D), BF16), pltpu.VMEM((rows, H), BF16), pltpu.VMEM((rows, H), BF16),
                        pltpu.VMEM((rows, D), F32), pltpu.VMEM((8,) + TILE, F32), pltpu.VMEM((4, 1024, 1024), BF16),
                        pltpu.SemaphoreType.DMA((4,))],
        compiler_params=pltpu.CompilerParams(vmem_limit_bytes=48 * 2**20),
        cost_estimate=pl.CostEstimate(flops=5 * 2 * 896 * 1024 * 1024, bytes_accessed=24 * 2**20, transcendentals=2 * 896 * 1024),
        name="forward",
    )(place, t_index, bucket_id, bucket_count, clean, noise, w1, w2, t1, t2)


def first_grad(place, grad_out, gate, inputs, w2):
    return pl.pallas_call(
        first_kernel,
        out_shape=(tiles(512), tiles(512)),
        in_specs=[SMEM] + [VMEM] * 4,
        out_specs=(VMEM,) * 2,
        scratch_shapes=[pltpu.VMEM((896, 256), BF16)],
        compiler_params=pltpu.CompilerParams(vmem_limit_bytes=32 * 2**20),
        cost_estimate=pl.CostEstimate(flops=2 * 2 * 896 * 1024 * 1024, bytes_accessed=12 * 2**20, transcendentals=0),
        name="first_grad",
    )(place, grad_out, gate, inputs, w2)


def call(kernel, outs, ins, vmem_mib, name, flops, moved):
    return pl.pallas_call(
        kernel,
        out_shape=outs,
        in_specs=[SMEM] + [VMEM] * (len(ins) - 1),
        out_specs=tuple(VMEM for _ in outs),
        compiler_params=pltpu.CompilerParams(vmem_limit_bytes=vmem_mib * 2**20),
        cost_estimate=pl.CostEstimate(flops=flops, bytes_accessed=moved, transcendentals=0),
        name=name,
    )(*ins)


def core_sum_kernel(place, keep, came, *pieces, with_bucket):
    for k in range(4):
        x, y = (place[1] + k) % 4, (place[2] + k) % 4
        at = pl.ds(pl.multiple_of(x * 64, 64), 64)
        pieces[k][pl.ds(0, 64)] = keep[at] + came[at]
        at = pl.ds(pl.multiple_of(256 + y * 64, 64), 64)
        pieces[4 + k][...] = keep[at] + came[at]
        if with_bucket:
            pieces[k][64] = keep[512] + came[512]


def core_sum(place, keep, came, with_bucket):
    outs = tuple(tiles(65 if with_bucket else 64) for _ in range(4)) + tuple(tiles(64) for _ in range(4))
    return call(functools.partial(core_sum_kernel, with_bucket=with_bucket), outs, (place, keep, came),
                10, "core_sum", 2**19, 6 * 2**20)


def send_all(pieces, axis):
    return [pieces[0]] + [lax.ppermute(pieces[k], axis, [(i, (i + k) % 4) for i in range(4)]) for k in range(1, 4)]


def exchange(pieces, axis, other):
    return send_all(pieces[:4], axis) + send_all(pieces[4:], other)


def plane_sum_kernel(place, *refs):
    second, first, pieces = refs[:8], refs[8:16], refs[16:]
    for k in range(4):
        x, y = (place[1] + k) % 4, (place[2] + k) % 4
        at = pl.ds(pl.multiple_of(y * 16, 16), 16)
        pieces[k][pl.ds(0, 16)] = (second[0][at] + second[1][at]) + (second[2][at] + second[3][at])
        pieces[k][pl.ds(16, 16)] = (first[0][at] + first[1][at]) + (first[2][at] + first[3][at])
        pieces[k][32] = (second[0][64] + second[1][64]) + (second[2][64] + second[3][64])
        at = pl.ds(pl.multiple_of(x * 16, 16), 16)
        pieces[4 + k][pl.ds(0, 16)] = (second[4][at] + second[5][at]) + (second[6][at] + second[7][at])
        pieces[4 + k][pl.ds(16, 16)] = (first[4][at] + first[5][at]) + (first[6][at] + first[7][at])


def plane_sum(place, second, first):
    outs = (tiles(33),) * 4 + (tiles(32),) * 4
    return call(plane_sum_kernel, outs, (place, *second, *first), 10, "plane_sum", 2**20, 5 * 2**20)


def line_sum_kernel(place, *refs):
    pieces, out = refs[:8], refs[8]
    for half in range(2):
        a, b, c, d = pieces[4 * half: 4 * half + 4]
        for g in range(2):
            for t in range(2):
                at = pl.ds(g * 16 + t * 8, 8)
                out[:, g * 4 + half * 2 + t] = (a[at] + b[at]) + (c[at] + d[at])
    bucket = (pieces[0][32] + pieces[1][32]) + (pieces[2][32] + pieces[3][32])
    for z in range(8):
        out[z, 8] = bucket


def line_sum(place, pieces):
    outs = (jax.ShapeDtypeStruct((8, 9, 8, 128), F32),)
    return call(line_sum_kernel, outs, (place, *pieces), 4, "line_sum", 2**18, 2**20)[0]


def last_sum_kernel(place, came, first, second, bucket):
    total = ((came[0] + came[1]) + (came[2] + came[3])) + ((came[4] + came[5]) + (came[6] + came[7]))
    for g, ref in enumerate((second, first)):
        for t in range(4):
            tile = total[g * 4 + t]
            ref[:, t * 256: t * 256 + 128] = tile[:4]
            ref[:, t * 256 + 128: t * 256 + 256] = tile[4:]
    bucket[...] = jnp.sum(total[8], axis=0, keepdims=True)


def last_sum(place, came):
    outs = (jax.ShapeDtypeStruct((4, 1024), F32), jax.ShapeDtypeStruct((4, 1024), F32), jax.ShapeDtypeStruct((1, 128), F32))
    return call(last_sum_kernel, outs, (place, came), 2, "last_sum", 2**16, 2**19)


def other_core(array):
    return lax.ppermute(array, "dp_2", [(0, 1), (1, 0)])


def local(clean, noise, t_index, bucket_id, bucket_count, w_first, w_second, teacher_first, teacher_second):
    rows = clean.shape[0] * clean.shape[1]
    total = clean.shape[0] * lax.axis_size(DP_OUTER)
    place = jnp.stack([lax.axis_index("dp_2"), lax.axis_index("outer"), lax.axis_index("dp_0")]).astype(jnp.int32)
    keep_s, send_s, grad_out, gate, inputs = forward(
        place, t_index, bucket_id, bucket_count, clean.reshape(rows, D), noise.reshape(rows, D),
        w_first, w_second, teacher_first, teacher_second, total)
    came_s = other_core(send_s)
    keep_f, send_f = first_grad(place, grad_out, gate, inputs, w_second)
    came_f = other_core(send_f)
    second = exchange(core_sum(place, keep_s, came_s, True), "outer", "dp_0")
    first = exchange(core_sum(place, keep_f, came_f, False), "outer", "dp_0")
    pieces = exchange(plane_sum(place, second, first), "dp_0", "outer")
    came = lax.all_to_all(line_sum(place, pieces), "dp_1", 0, 0, tiled=True)
    first_rows, second_rows, bucket = last_sum(place, came)
    return first_rows, second_rows, bucket[0, :16]


def solution(mesh):
    split = Mesh(mesh.devices.reshape(4, 8, 2, mesh.shape["outer"]), ("dp_0", "dp_1", "dp_2", "outer"))
    placed = (P(DP_OUTER, None, None), P(DP_OUTER, None, None), P(DP_OUTER), P(DP_OUTER), P(), P(), P(), P(), P())
    return jax.shard_map(local, mesh=split, in_specs=placed,
                         out_specs=(P(DP_OUTER, None), P(DP_OUTER, None), P()), check_vma=False)
```

```python
import functools, math
import jax, jax.numpy as jnp
from jax import lax
from jax.experimental import pallas as pl
from jax.experimental.pallas import tpu as pltpu
from jax.sharding import Mesh
from jax.sharding import PartitionSpec as P

DP_OUTER = ("dp_0", "dp_1", "dp_2", "outer")

STEPS = 1280
sigma_floor = 0.002
sigma_ceiling = 80.0
sigma_data = 0.5
huber_scale = 0.00054
rho_power = 7.0
F32, BF16 = jnp.float32, jnp.bfloat16
LAT, PATCHES, D, H, BUCKETS = 8, 112, 1024, 1024, 16
ROWS = LAT * PATCHES
TILE = (8, 128)
TN = 256
MB = 896
CORE, FIRST_AT, SECOND_AT, T_INDEX, BUCKET_ID, BUCKET_COUNT = 0, 1, 2, 3, 11, 19
VMEM = pl.BlockSpec(memory_space=pltpu.VMEM)
SMEM = pl.BlockSpec(memory_space=pltpu.SMEM)
ANY = pl.BlockSpec(memory_space=pltpu.HBM)


def rows_from(values):
    row = lax.broadcasted_iota(jnp.int32, TILE, 0)
    out = jnp.full(TILE, values[0])
    for k in range(1, len(values)):
        out = jnp.where(row == k, values[k], out)
    return out


def plan(index):
    ramp = index.astype(F32) / (STEPS - 1)
    top = sigma_ceiling ** (1.0 / rho_power)
    bottom = sigma_floor ** (1.0 / rho_power)
    base = top + ramp * (bottom - top)
    square = base * base
    fourth = square * square
    return fourth * square * base


def scale_factors(s):
    skip = sigma_data**2 / ((s - sigma_floor) ** 2 + sigma_data**2)
    scale = jnp.sqrt(s * s + sigma_data**2)
    return skip, (s - sigma_floor) * sigma_data / scale, 1.0 / scale


def sigmoid(x):
    return 0.5 * jnp.tanh(0.5 * x) + 0.5


def transposed_dot(a, b):
    return lax.dot_general(a, b, (((0,), (0,)), ((), ())), preferred_element_type=F32)


def store_routed(block, y, t, color, ref):
    v = block.reshape(32, 8, 256)
    left, right = v[:, :, :128], v[:, :, 128:]
    halves = (
        jnp.concatenate([left[:, :4], right[:, :4]], axis=1),
        jnp.concatenate([left[:, 4:], right[:, 4:]], axis=1),
    )
    for x in range(4):
        pieces = halves[x % 2].reshape(8, 2, 2, 8, 128)[:, :, x // 2]
        place = jnp.where(color == 0, x * 4 + y, y * 4 + x)
        for c in range(2):
            ref[pl.ds((place * 2 + t) * 16 + c * 8, 8)] = pieces[:, c]


def weight_gradient(left, right, color, ref):
    for t in range(2):
        cols = pl.ds(pl.multiple_of((2 * color + t) * TN, TN), TN)

        def part(y, _):
            block = transposed_dot(left[:, pl.ds(pl.multiple_of(y * 256, 256), 256)], right[:, cols])
            store_routed(block, y, t, color, ref)
            return 0

        lax.fori_loop(0, 4, part, 0)


def forward_kernel(info, clean_hbm, noise_hbm, w1, w2, t1, t2,
                   send, bucket, grad_out, gate, inputs, act_hi,
                   clean, noise, in_lo, act_lo, diff, coef, wbuf, field_sems, sems, *, total):
    fields = []
    for lat in range(LAT):
        rows = pl.ds(lat * PATCHES, PATCHES)
        fields.append((pltpu.make_async_copy(clean_hbm.at[lat], clean.at[rows], field_sems.at[0, lat]),
                       pltpu.make_async_copy(noise_hbm.at[lat], noise.at[rows], field_sems.at[1, lat])))
    copies = [pltpu.make_async_copy(src, wbuf.at[k], sems.at[k]) for k, src in enumerate((w1, t1, w2, t2))]
    for pair in fields:
        pair[0].start()
        pair[1].start()
    for copy in copies:
        copy.start()
    hi_index = rows_from([info[T_INDEX + k] for k in range(LAT)])
    s_hi, s_lo = plan(hi_index), plan(hi_index + 1)
    skip_hi, out_hi, in_scale_hi = scale_factors(s_hi)
    skip_lo, out_lo, in_scale_lo = scale_factors(s_lo)
    coef[0] = in_scale_hi
    coef[1] = in_scale_hi * s_hi
    coef[2] = in_scale_lo
    coef[3] = in_scale_lo * s_lo
    coef[4] = s_hi
    coef[5] = s_lo
    coef[6] = out_hi
    coef[7] = out_lo
    coef[8] = skip_hi
    coef[9] = skip_lo

    def one(k, lat):
        return coef[k, pl.ds(lat, 1), 0:1]

    for lat in range(LAT):
        rows = pl.ds(lat * PATCHES, PATCHES)
        fields[lat][0].wait()
        fields[lat][1].wait()
        c, n = clean[rows, :].astype(F32), noise[rows, :].astype(F32)
        inputs[rows, :] = (one(0, lat) * (c + one(4, lat) * n)).astype(BF16)
        in_lo[rows, :] = (one(2, lat) * (c + one(5, lat) * n)).astype(BF16)
    copies[0].wait()
    copies[1].wait()
    NB = ROWS // MB

    def hidden(i, _):
        rows = pl.ds(pl.multiple_of((i % NB) * MB, MB), MB)
        cols = pl.ds(pl.multiple_of((i // NB) * TN, TN), TN)
        pre = jnp.dot(inputs[rows, :], wbuf[0, :, cols], preferred_element_type=F32)
        sig = sigmoid(pre)
        act_hi[rows, cols] = (pre * sig).astype(BF16)
        gate[rows, cols] = sig * (1.0 + pre * (1.0 - sig))
        pre = jnp.dot(in_lo[rows, :], wbuf[1, :, cols], preferred_element_type=F32)
        act_lo[rows, cols] = (pre * sigmoid(pre)).astype(BF16)
        return 0
    lax.fori_loop(0, NB * 4, hidden, 0)
    copies[2].wait()
    copies[3].wait()
    row = lax.broadcasted_iota(jnp.int32, TILE, 0)

    def outer(i, sums):
        rows = pl.ds(pl.multiple_of((i % NB) * MB, MB), MB)
        cols = pl.ds(pl.multiple_of((i // NB) * TN, TN), TN)
        online = jnp.dot(act_hi[rows, :], wbuf[2, :, cols], preferred_element_type=F32)
        target = jnp.dot(act_lo[rows, :], wbuf[3, :, cols], preferred_element_type=F32)
        for k in range(MB // PATCHES):
            lat = (i % NB) * (MB // PATCHES) + k
            r = pl.ds(lat * PATCHES, PATCHES)
            s = slice(k * PATCHES, (k + 1) * PATCHES)
            c, n = clean[r, cols].astype(F32), noise[r, cols].astype(F32)
            on = one(8, lat) * (c + one(4, lat) * n) + one(6, lat) * online[s]
            tg = one(9, lat) * (c + one(5, lat) * n) + one(7, lat) * target[s]
            d = on - tg
            diff[r, cols] = d
            sq = jnp.sum((d * d).reshape(PATCHES // 8, 8, TN), axis=0)
            sq = sq[:, :128] + sq[:, 128:]
            sums = sums + jnp.where(row == lat, jnp.sum(sq, axis=0, keepdims=True), 0.0)
        return sums
    sums = lax.fori_loop(0, NB * 4, outer, jnp.zeros(TILE, F32))
    q = jnp.sum(sums, axis=1, keepdims=True)
    c2 = huber_scale * math.sqrt(PATCHES * D)
    root = jnp.sqrt(q + c2**2)
    distance = root - c2
    count = rows_from([info[BUCKET_COUNT + info[BUCKET_ID + k]].astype(F32) for k in range(LAT)])
    weight = s_lo / (s_hi - s_lo) / jnp.sqrt(count) / total
    lane = lax.broadcasted_iota(jnp.int32, TILE, 1)
    part = jnp.where(lane == rows_from([info[BUCKET_ID + k] for k in range(LAT)]), weight * distance, 0.0)
    bucket[...] = part
    send[512] = part
    coef[10] = weight / root

    def grad(lat, _):
        rows = pl.ds(lat * PATCHES, PATCHES)
        grad_out[rows, :] = (one(10, lat) * diff[rows, :] * one(6, lat)).astype(BF16)
        return 0
    lax.fori_loop(0, LAT, grad, 0)
    weight_gradient(act_hi, grad_out, 1 - info[CORE], send)


def second_kernel(info, act_hi, grad_out, keep):
    weight_gradient(act_hi, grad_out, info[CORE], keep)


def first_kernel(info, grad_out, gate, inputs, w2, out, grad_pre, *, color_flip):
    color = 1 - info[CORE] if color_flip else info[CORE]
    for t in range(2):
        cols = pl.ds(pl.multiple_of((2 * color + t) * TN, TN), TN)
        for m in range(2):
            rows = slice(m * 448, (m + 1) * 448)
            back = lax.dot_general(grad_out[rows, :], w2[cols, :], (((1,), (1,)), ((), ())), preferred_element_type=F32)
            grad_pre[rows, :] = (back * gate[rows, cols]).astype(BF16)

        def first(y, _):
            block = transposed_dot(inputs[:, pl.ds(pl.multiple_of(y * 256, 256), 256)], grad_pre[...])
            store_routed(block, y, t, color, out)
            return 0

        lax.fori_loop(0, 4, first, 0)


def tiles(n):
    return jax.ShapeDtypeStruct((n, 8, 128), F32)


def bf16(*shape):
    return jax.ShapeDtypeStruct(shape, BF16)


PRODUCT = 2 * ROWS * D * H


def forward(info, clean, noise, w1, w2, t1, t2, total):
    return pl.pallas_call(
        functools.partial(forward_kernel, total=total),
        out_shape=(pltpu.VMEM((513, 8, 128), F32), pltpu.VMEM(TILE, F32), pltpu.VMEM((ROWS, D), BF16),
                   pltpu.VMEM((ROWS, H), F32), pltpu.VMEM((ROWS, D), BF16), pltpu.VMEM((ROWS, H), BF16)),
        in_specs=[SMEM] + [ANY] * 6,
        out_specs=(VMEM,) * 6,
        scratch_shapes=[pltpu.VMEM((ROWS, D), BF16), pltpu.VMEM((ROWS, D), BF16), pltpu.VMEM((ROWS, D), BF16),
                        pltpu.VMEM((ROWS, H), BF16), pltpu.VMEM((ROWS, D), F32), pltpu.VMEM((11,) + TILE, F32),
                        pltpu.VMEM((4, D, H), BF16), pltpu.SemaphoreType.DMA((2, LAT)), pltpu.SemaphoreType.DMA((4,))],
        compiler_params=pltpu.CompilerParams(vmem_limit_bytes=51 * 2**20),
        cost_estimate=pl.CostEstimate(flops=9 * PRODUCT // 2, bytes_accessed=24 * 2**20, transcendentals=2 * ROWS * H),
        name="forward",
    )(info, clean, noise, w1, w2, t1, t2)


def second_grad(info, act_hi, grad_out):
    return pl.pallas_call(
        second_kernel,
        out_shape=pltpu.VMEM((512, 8, 128), F32),
        in_specs=[SMEM, VMEM, VMEM],
        out_specs=VMEM,
        compiler_params=pltpu.CompilerParams(vmem_limit_bytes=16 * 2**20),
        cost_estimate=pl.CostEstimate(flops=PRODUCT // 2, bytes_accessed=4 * 2**20, transcendentals=0),
        name="second_grad",
    )(info, act_hi, grad_out)


def first_grad(info, grad_out, gate, inputs, w2, color_flip, rows=pltpu.VMEM((512, 8, 128), F32)):
    return pl.pallas_call(
        functools.partial(first_kernel, color_flip=color_flip),
        out_shape=rows,
        in_specs=[SMEM] + [VMEM] * 4,
        out_specs=VMEM,
        scratch_shapes=[pltpu.VMEM((ROWS, TN), BF16)],
        compiler_params=pltpu.CompilerParams(vmem_limit_bytes=20 * 2**20),
        cost_estimate=pl.CostEstimate(flops=PRODUCT, bytes_accessed=8 * 2**20, transcendentals=0),
        name="first_grad",
    )(info, grad_out, gate, inputs, w2)


def call(kernel, outs, ins, vmem_mib, name, flops, moved):
    return pl.pallas_call(
        kernel,
        out_shape=outs,
        in_specs=[SMEM] + [VMEM] * (len(ins) - 1),
        out_specs=tuple(VMEM for _ in outs),
        compiler_params=pltpu.CompilerParams(vmem_limit_bytes=vmem_mib * 2**20),
        cost_estimate=pl.CostEstimate(flops=flops, bytes_accessed=moved, transcendentals=0),
        name=name,
    )(*ins)


def core_sum_kernel(info, keep, came, *rest, with_bucket):
    bucket, pieces = (rest[0], rest[1:]) if with_bucket else (None, rest)
    for k in range(4):
        p = (info[FIRST_AT] + k) % 4
        at = pl.ds(pl.multiple_of(p * 128, 128), 128)
        pieces[k][pl.ds(0, 128)] = keep[at] + came[at]
        if with_bucket:
            pieces[k][128] = bucket[...] + came[512]


def core_sum(info, keep, came, bucket=None):
    outs = tuple(tiles(128 if bucket is None else 129) for _ in range(4))
    ins = (info, keep, came) if bucket is None else (info, keep, came, bucket)
    return call(functools.partial(core_sum_kernel, with_bucket=bucket is not None), outs, ins,
                10, "core_sum", 2**19, 6 * 2**20)


def shift_pairs(k, x_on_core):
    pairs = []
    for y in range(4):
        for z in range(8):
            for core in range(2):
                for x in range(4):
                    to = (y, z, core, (x + k) % 4) if core == x_on_core else ((y + k) % 4, z, core, x)
                    pairs.append((((y * 8 + z) * 2 + core) * 4 + x, ((to[0] * 8 + to[1]) * 2 + to[2]) * 4 + to[3]))
    return pairs


def exchange(pieces, x_on_core):
    return [pieces[0]] + [lax.ppermute(pieces[k], DP_OUTER, shift_pairs(k, x_on_core)) for k in range(1, 4)]


def plane_sum_kernel(info, *refs):
    second, first, pieces = refs[:4], refs[4:8], refs[8:]
    for k in range(4):
        q = (info[SECOND_AT] + k) % 4
        at = pl.ds(pl.multiple_of(q * 32, 32), 32)
        pieces[k][pl.ds(0, 32)] = (second[0][at] + second[1][at]) + (second[2][at] + second[3][at])
        pieces[k][pl.ds(32, 32)] = (first[0][at] + first[1][at]) + (first[2][at] + first[3][at])
        pieces[k][64] = (second[0][128] + second[1][128]) + (second[2][128] + second[3][128])


def plane_sum(info, second, first):
    return call(plane_sum_kernel, (tiles(65),) * 4, (info, *second, *first), 10, "plane_sum", 2**20, 5 * 2**20)


def line_sum_kernel(info, a, b, c, d, out):
    for g in range(2):
        for t in range(2):
            for core in range(2):
                at = pl.ds(g * 32 + t * 16 + core * 8, 8)
                out[:, core, 2 * g + t] = (a[at] + b[at]) + (c[at] + d[at])
    bucket = (a[64] + b[64]) + (c[64] + d[64])
    for z in range(8):
        for core in range(2):
            out[z, core, 4] = bucket


def line_sum(info, pieces):
    outs = (jax.ShapeDtypeStruct((8, 2, 5, 8, 128), F32),)
    return call(line_sum_kernel, outs, (info, *pieces), 4, "line_sum", 2**18, 2**20)[0]


def last_sum_kernel(info, came, first, second, bucket):
    def total(color, at):
        v = [came[2 * z + color, at] for z in range(8)]
        return ((v[0] + v[1]) + (v[2] + v[3])) + ((v[4] + v[5]) + (v[6] + v[7]))

    for g, ref in enumerate((second, first)):
        for color in range(2):
            for t in range(2):
                tile = total(color, 2 * g + t)
                at = (2 * color + t) * 256
                ref[:, at: at + 128] = tile[:4]
                ref[:, at + 128: at + 256] = tile[4:]
    bucket[...] = jnp.sum(total(0, 4), axis=0, keepdims=True)


def last_sum(info, came):
    outs = (jax.ShapeDtypeStruct((4, 1024), F32), jax.ShapeDtypeStruct((4, 1024), F32), jax.ShapeDtypeStruct((1, 128), F32))
    return call(last_sum_kernel, outs, (info, came), 2, "last_sum", 2**16, 2**19)


def other_core(array):
    return lax.ppermute(array, "dp_2", [(0, 1), (1, 0)])


def local(clean, noise, t_index, bucket_id, bucket_count, w_first, w_second, teacher_first, teacher_second):
    total = clean.shape[0] * lax.axis_size(DP_OUTER)
    core, x, y = lax.axis_index("dp_2"), lax.axis_index("outer"), lax.axis_index("dp_0")
    place = jnp.stack([core, jnp.where(core == 0, x, y), jnp.where(core == 0, y, x)]).astype(jnp.int32)
    info = jnp.concatenate([place, t_index, bucket_id, bucket_count])
    send_s, bucket, grad_out, gate, inputs, act_hi = forward(
        info, clean, noise, w_first, w_second, teacher_first, teacher_second, total)
    came_s = other_core(send_s)
    keep_s = second_grad(info, act_hi, grad_out)
    send_f = first_grad(info, grad_out, gate, inputs, w_second, True)
    came_f = other_core(send_f)
    second = exchange(core_sum(info, keep_s, came_s, bucket), 0)
    keep_f = first_grad(info, grad_out, gate, inputs, w_second, False)
    first = exchange(core_sum(info, keep_f, came_f), 0)
    pieces = exchange(plane_sum(info, second, first), 1)
    came = lax.all_to_all(line_sum(info, pieces).reshape(16, 5, 8, 128), ("dp_1", "dp_2"), 0, 0, tiled=True)
    first_rows, second_rows, losses = last_sum(info, came)
    return first_rows, second_rows, losses[0, :BUCKETS]


def solution(mesh):
    split = Mesh(mesh.devices.reshape(4, 8, 2, mesh.shape["outer"]), DP_OUTER)
    placed = (P(DP_OUTER, None, None), P(DP_OUTER, None, None), P(DP_OUTER), P(DP_OUTER), P(), P(), P(), P(), P())
    return jax.shard_map(local, mesh=split, in_specs=placed,
                         out_specs=(P(DP_OUTER, None), P(DP_OUTER, None), P()), check_vma=False)
```

```python
import functools, math
import jax, jax.numpy as jnp
from jax import lax
from jax.experimental import pallas as pl
from jax.experimental.pallas import tpu as pltpu
from jax.sharding import Mesh
from jax.sharding import PartitionSpec as P

DP_OUTER = ("dp_0", "dp_1", "dp_2", "outer")

STEPS = 1280
sigma_floor = 0.002
sigma_ceiling = 80.0
sigma_data = 0.5
huber_scale = 0.00054
rho_power = 7.0
F32, BF16 = jnp.float32, jnp.bfloat16
LAT, PATCHES, D, H, BUCKETS = 8, 112, 1024, 1024, 16
ROWS = LAT * PATCHES
TILE = (8, 128)
TN = 256
MB = 448
CORE, FIRST_AT, SECOND_AT = 0, 1, 2
VMEM = pl.BlockSpec(memory_space=pltpu.VMEM)
SMEM = pl.BlockSpec(memory_space=pltpu.SMEM)
ANY = pl.BlockSpec(memory_space=pltpu.HBM)


def rows_from(values):
    row = lax.broadcasted_iota(jnp.int32, TILE, 0)
    out = jnp.full(TILE, values[0])
    for k in range(1, len(values)):
        out = jnp.where(row == k, values[k], out)
    return out


def plan(index):
    ramp = index.astype(F32) / (STEPS - 1)
    top = sigma_ceiling ** (1.0 / rho_power)
    bottom = sigma_floor ** (1.0 / rho_power)
    base = top + ramp * (bottom - top)
    square = base * base
    fourth = square * square
    return fourth * square * base


def scale_factors(s):
    skip = sigma_data**2 / ((s - sigma_floor) ** 2 + sigma_data**2)
    scale = jnp.sqrt(s * s + sigma_data**2)
    return skip, (s - sigma_floor) * sigma_data / scale, 1.0 / scale


def sigmoid(x):
    return 0.5 * jnp.tanh(0.5 * x) + 0.5


def transposed_dot(a, b):
    return lax.dot_general(a, b, (((0,), (0,)), ((), ())), preferred_element_type=F32)


def store_routed(block, y, t, color, ref):
    v = block.reshape(32, 8, 256)
    left, right = v[:, :, :128], v[:, :, 128:]
    halves = (
        jnp.concatenate([left[:, :4], right[:, :4]], axis=1),
        jnp.concatenate([left[:, 4:], right[:, 4:]], axis=1),
    )
    for x in range(4):
        pieces = halves[x % 2].reshape(8, 2, 2, 8, 128)[:, :, x // 2]
        place = jnp.where(color == 0, x * 4 + y, y * 4 + x)
        for c in range(2):
            ref[pl.ds((place * 2 + t) * 16 + c * 8, 8)] = pieces[:, c]


def weight_gradient(left, right, right_cols, color, ref):
    def part(y, _):
        block = transposed_dot(left[:, pl.ds(pl.multiple_of(y * 256, 256), 256)], right[:, right_cols])
        for t in range(2):
            store_routed(block[:, t * TN:(t + 1) * TN], y, t, color, ref)
        return 0

    lax.fori_loop(0, 4, part, 0, unroll=True)


def half(color):
    return pl.ds(pl.multiple_of(color * 512, 512), 512)


def forward_kernel(place_hbm, t_index_hbm, bucket_id_hbm, bucket_count_hbm, clean_hbm, noise_hbm, w1, w2, t1, t2,
                   send, bucket, grad_out, gate, inputs, act_hi,
                   clean, noise, in_lo, act_lo, diff, coef, wbuf, place, t_index, bucket_id, bucket_count,
                   field_sems, sems, small_sems, *, total):
    small = [pltpu.make_async_copy(src, dst, small_sems.at[k]) for k, (src, dst) in enumerate((
        (place_hbm, place), (t_index_hbm, t_index), (bucket_id_hbm, bucket_id), (bucket_count_hbm, bucket_count)))]
    fields = []
    for lat in range(LAT):
        rows = pl.ds(lat * PATCHES, PATCHES)
        fields.append((pltpu.make_async_copy(clean_hbm.at[lat], clean.at[rows], field_sems.at[0, lat]),
                       pltpu.make_async_copy(noise_hbm.at[lat], noise.at[rows], field_sems.at[1, lat])))
    copies = [pltpu.make_async_copy(src, wbuf.at[k], sems.at[k]) for k, src in enumerate((w1, t1, w2, t2))]
    for copy in small:
        copy.start()
    for pair in fields:
        pair[0].start()
        pair[1].start()
    for copy in copies:
        copy.start()
    for copy in small:
        copy.wait()
    hi_index = rows_from([t_index[k] for k in range(LAT)])
    s_hi, s_lo = plan(hi_index), plan(hi_index + 1)
    skip_hi, out_hi, in_scale_hi = scale_factors(s_hi)
    skip_lo, out_lo, in_scale_lo = scale_factors(s_lo)
    coef[0] = in_scale_hi
    coef[1] = in_scale_lo
    coef[2] = s_hi
    coef[3] = s_lo
    coef[4] = out_hi
    coef[5] = out_lo
    coef[6] = skip_hi
    coef[7] = skip_lo

    def one(k, lat):
        return coef[k, lat:lat + 1, 0:1]

    def block_rows(lat):
        return slice(lat * PATCHES, (lat + 1) * PATCHES)

    def field(lat, side, ref):
        rows = block_rows(lat)
        c, n = clean[rows, :].astype(F32), noise[rows, :].astype(F32)
        ref[rows, :] = (one(side, lat) * (c + one(2 + side, lat) * n)).astype(BF16)

    for lat in range(LAT):
        fields[lat][0].wait()
        fields[lat][1].wait()
        field(lat, 0, inputs)
    copies[0].wait()
    for j in range(H // TN):
        cols = slice(j * TN, (j + 1) * TN)
        pre = jnp.dot(inputs[...], wbuf[0, :, cols], preferred_element_type=F32)
        sig = sigmoid(pre)
        act_hi[:, cols] = (pre * sig).astype(BF16)
        gate[:, cols] = sig * (1.0 + pre * (1.0 - sig))
        for lat in range(2 * j, 2 * j + 2):
            field(lat, 1, in_lo)
    copies[1].wait()
    for j in range(H // TN):
        cols = slice(j * TN, (j + 1) * TN)
        pre = jnp.dot(in_lo[...], wbuf[1, :, cols], preferred_element_type=F32)
        act_lo[:, cols] = (pre * sigmoid(pre)).astype(BF16)
    copies[2].wait()
    copies[3].wait()
    row = lax.broadcasted_iota(jnp.int32, TILE, 0)
    sums = jnp.zeros(TILE, F32)
    for j in range(D // TN):
        cols = slice(j * TN, (j + 1) * TN)
        for m in range(2):
            rows = slice(m * MB, (m + 1) * MB)
            online = jnp.dot(act_hi[rows, :], wbuf[2, :, cols], preferred_element_type=F32)
            target = jnp.dot(act_lo[rows, :], wbuf[3, :, cols], preferred_element_type=F32)
            for k in range(MB // PATCHES):
                lat = m * (MB // PATCHES) + k
                r, s = block_rows(lat), block_rows(k)
                c, n = clean[r, cols].astype(F32), noise[r, cols].astype(F32)
                on = one(6, lat) * (c + one(2, lat) * n) + one(4, lat) * online[s]
                tg = one(7, lat) * (c + one(3, lat) * n) + one(5, lat) * target[s]
                d = on - tg
                diff[r, cols] = d
                sq = jnp.sum((d * d).reshape(PATCHES // 8, 8, TN), axis=0)
                sq = sq[:, :128] + sq[:, 128:]
                sums = sums + jnp.where(row == lat, jnp.sum(sq, axis=0, keepdims=True), 0.0)
    q = jnp.sum(sums, axis=1, keepdims=True)
    c2 = huber_scale * math.sqrt(PATCHES * D)
    root = jnp.sqrt(q + c2**2)
    distance = root - c2
    count = rows_from([bucket_count[bucket_id[k]].astype(F32) for k in range(LAT)])
    weight = s_lo / (s_hi - s_lo) / jnp.sqrt(count) / total
    lane = lax.broadcasted_iota(jnp.int32, TILE, 1)
    part = jnp.where(lane == rows_from([bucket_id[k] for k in range(LAT)]), weight * distance, 0.0)
    bucket[...] = part
    send[512] = part
    coef[8] = out_hi * (weight / root)
    for lat in range(LAT):
        rows = block_rows(lat)
        grad_out[rows, :] = (one(8, lat) * diff[rows, :]).astype(BF16)
    color = 1 - place[CORE]
    weight_gradient(act_hi, grad_out, half(color), color, send)


def second_kernel(info, act_hi, grad_out, keep):
    weight_gradient(act_hi, grad_out, half(info[CORE]), info[CORE], keep)


def first_kernel(info, grad_out, gate, inputs, w2, out, grad_pre, *, color_flip):
    color = 1 - info[CORE] if color_flip else info[CORE]
    cols = half(color)

    def back(m, _):
        rows = pl.ds(pl.multiple_of(m * 224, 224), 224)
        product = lax.dot_general(grad_out[rows, :], w2[cols, :], (((1,), (1,)), ((), ())), preferred_element_type=F32)
        grad_pre[rows, :] = (product * gate[rows, cols]).astype(BF16)
        return 0

    lax.fori_loop(0, 4, back, 0, unroll=True)
    weight_gradient(inputs, grad_pre, slice(None), color, out)


def tiles(n):
    return jax.ShapeDtypeStruct((n, 8, 128), F32)


def bf16(*shape):
    return jax.ShapeDtypeStruct(shape, BF16)


PRODUCT = 2 * ROWS * D * H


def forward(info, t_index, bucket_id, bucket_count, clean, noise, w1, w2, t1, t2, total):
    return pl.pallas_call(
        functools.partial(forward_kernel, total=total),
        out_shape=(pltpu.VMEM((513, 8, 128), F32), pltpu.VMEM(TILE, F32), pltpu.VMEM((ROWS, D), BF16),
                   pltpu.VMEM((ROWS, H), F32), pltpu.VMEM((ROWS, D), BF16), pltpu.VMEM((ROWS, H), BF16)),
        in_specs=[ANY] * 10,
        out_specs=(VMEM,) * 6,
        scratch_shapes=[pltpu.VMEM((ROWS, D), BF16), pltpu.VMEM((ROWS, D), BF16), pltpu.VMEM((ROWS, D), BF16),
                        pltpu.VMEM((ROWS, H), BF16), pltpu.VMEM((ROWS, D), F32), pltpu.VMEM((9,) + TILE, F32),
                        pltpu.VMEM((4, D, H), BF16), pltpu.SMEM((3,), jnp.int32), pltpu.SMEM((LAT,), jnp.int32),
                        pltpu.SMEM((LAT,), jnp.int32), pltpu.SMEM((BUCKETS,), jnp.int32),
                        pltpu.SemaphoreType.DMA((2, LAT)), pltpu.SemaphoreType.DMA((4,)), pltpu.SemaphoreType.DMA((4,))],
        compiler_params=pltpu.CompilerParams(vmem_limit_bytes=51 * 2**20),
        cost_estimate=pl.CostEstimate(flops=9 * PRODUCT // 2, bytes_accessed=24 * 2**20, transcendentals=2 * ROWS * H),
        name="forward",
    )(info, t_index, bucket_id, bucket_count, clean, noise, w1, w2, t1, t2)


def second_grad(info, act_hi, grad_out):
    return pl.pallas_call(
        second_kernel,
        out_shape=pltpu.VMEM((512, 8, 128), F32),
        in_specs=[SMEM, VMEM, VMEM],
        out_specs=VMEM,
        compiler_params=pltpu.CompilerParams(vmem_limit_bytes=16 * 2**20),
        cost_estimate=pl.CostEstimate(flops=PRODUCT // 2, bytes_accessed=4 * 2**20, transcendentals=0),
        name="second_grad",
    )(info, act_hi, grad_out)


def first_grad(info, grad_out, gate, inputs, w2, color_flip, rows=pltpu.VMEM((512, 8, 128), F32)):
    return pl.pallas_call(
        functools.partial(first_kernel, color_flip=color_flip),
        out_shape=rows,
        in_specs=[SMEM] + [VMEM] * 4,
        out_specs=VMEM,
        scratch_shapes=[pltpu.VMEM((ROWS, 512), BF16)],
        compiler_params=pltpu.CompilerParams(vmem_limit_bytes=20 * 2**20),
        cost_estimate=pl.CostEstimate(flops=PRODUCT, bytes_accessed=8 * 2**20, transcendentals=0),
        name="first_grad",
    )(info, grad_out, gate, inputs, w2)


def call(kernel, outs, ins, vmem_mib, name, flops, moved):
    return pl.pallas_call(
        kernel,
        out_shape=outs,
        in_specs=[SMEM] + [VMEM] * (len(ins) - 1),
        out_specs=tuple(VMEM for _ in outs),
        compiler_params=pltpu.CompilerParams(vmem_limit_bytes=vmem_mib * 2**20),
        cost_estimate=pl.CostEstimate(flops=flops, bytes_accessed=moved, transcendentals=0),
        name=name,
    )(*ins)


def core_sum_kernel(info, keep, came, *rest, with_bucket):
    bucket, pieces = (rest[0], rest[1:]) if with_bucket else (None, rest)
    for k in range(4):
        p = (info[FIRST_AT] + k) % 4
        at = pl.ds(pl.multiple_of(p * 128, 128), 128)
        pieces[k][pl.ds(0, 128)] = keep[at] + came[at]
        if with_bucket:
            pieces[k][128] = bucket[...] + came[512]


def core_sum(info, keep, came, bucket=None):
    outs = tuple(tiles(128 if bucket is None else 129) for _ in range(4))
    ins = (info, keep, came) if bucket is None else (info, keep, came, bucket)
    return call(functools.partial(core_sum_kernel, with_bucket=bucket is not None), outs, ins,
                10, "core_sum", 2**19, 6 * 2**20)


def shift_pairs(k, x_on_core):
    pairs = []
    for y in range(4):
        for z in range(8):
            for core in range(2):
                for x in range(4):
                    to = (y, z, core, (x + k) % 4) if core == x_on_core else ((y + k) % 4, z, core, x)
                    pairs.append((((y * 8 + z) * 2 + core) * 4 + x, ((to[0] * 8 + to[1]) * 2 + to[2]) * 4 + to[3]))
    return pairs


def exchange(pieces, x_on_core):
    return [pieces[0]] + [lax.ppermute(pieces[k], DP_OUTER, shift_pairs(k, x_on_core)) for k in (1, 3, 2)]


def plane_sum_kernel(info, *refs):
    second, first, pieces = refs[:4], refs[4:8], refs[8:]
    for k in range(4):
        q = (info[SECOND_AT] + k) % 4
        at = pl.ds(pl.multiple_of(q * 32, 32), 32)
        pieces[k][pl.ds(0, 32)] = (second[0][at] + second[1][at]) + (second[2][at] + second[3][at])
        pieces[k][pl.ds(32, 32)] = (first[0][at] + first[1][at]) + (first[2][at] + first[3][at])
        pieces[k][64] = (second[0][128] + second[1][128]) + (second[2][128] + second[3][128])


def plane_sum(info, second, first):
    return call(plane_sum_kernel, (tiles(65),) * 4, (info, *second, *first), 10, "plane_sum", 2**20, 5 * 2**20)


def line_sum_kernel(info, a, b, c, d, out):
    for g in range(2):
        for t in range(2):
            for core in range(2):
                at = pl.ds(g * 32 + t * 16 + core * 8, 8)
                out[:, core, 2 * g + t] = (a[at] + b[at]) + (c[at] + d[at])
    bucket = (a[64] + b[64]) + (c[64] + d[64])
    for z in range(8):
        for core in range(2):
            out[z, core, 4] = bucket


def line_sum(info, pieces):
    outs = (jax.ShapeDtypeStruct((8, 2, 5, 8, 128), F32),)
    return call(line_sum_kernel, outs, (info, *pieces), 4, "line_sum", 2**18, 2**20)[0]


def last_sum_kernel(info, came, first, second, bucket):
    def total(color, at):
        v = [came[2 * z + color, at] for z in range(8)]
        return ((v[0] + v[1]) + (v[2] + v[3])) + ((v[4] + v[5]) + (v[6] + v[7]))

    for g, ref in enumerate((second, first)):
        for color in range(2):
            for t in range(2):
                tile = total(color, 2 * g + t)
                at = (2 * color + t) * 256
                ref[:, at: at + 128] = tile[:4]
                ref[:, at + 128: at + 256] = tile[4:]
    bucket[...] = jnp.sum(total(0, 4), axis=0, keepdims=True)


def last_sum(info, came):
    outs = (jax.ShapeDtypeStruct((4, 1024), F32), jax.ShapeDtypeStruct((4, 1024), F32), jax.ShapeDtypeStruct((1, 128), F32))
    return call(last_sum_kernel, outs, (info, came), 2, "last_sum", 2**16, 2**19)


def other_core(array):
    return lax.ppermute(array, "dp_2", [(0, 1), (1, 0)])


def local(clean, noise, t_index, bucket_id, bucket_count, w_first, w_second, teacher_first, teacher_second):
    total = clean.shape[0] * lax.axis_size(DP_OUTER)
    core, x, y = lax.axis_index("dp_2"), lax.axis_index("outer"), lax.axis_index("dp_0")
    info = jnp.stack([core, jnp.where(core == 0, x, y), jnp.where(core == 0, y, x)]).astype(jnp.int32)
    send_s, bucket, grad_out, gate, inputs, act_hi = forward(
        info, t_index, bucket_id, bucket_count, clean, noise, w_first, w_second, teacher_first, teacher_second, total)
    came_s = other_core(send_s)
    keep_s = second_grad(info, act_hi, grad_out)
    send_f = first_grad(info, grad_out, gate, inputs, w_second, True)
    came_f = other_core(send_f)
    second = exchange(core_sum(info, keep_s, came_s, bucket), 0)
    keep_f = first_grad(info, grad_out, gate, inputs, w_second, False)
    first = exchange(core_sum(info, keep_f, came_f), 0)
    pieces = exchange(plane_sum(info, second, first), 1)
    came = lax.all_to_all(line_sum(info, pieces).reshape(16, 5, 8, 128), ("dp_1", "dp_2"), 0, 0, tiled=True)
    first_rows, second_rows, losses = last_sum(info, came)
    return first_rows, second_rows, losses[0, :BUCKETS]


def solution(mesh):
    split = Mesh(mesh.devices.reshape(4, 8, 2, mesh.shape["outer"]), DP_OUTER)
    placed = (P(DP_OUTER, None, None), P(DP_OUTER, None, None), P(DP_OUTER), P(DP_OUTER), P(), P(), P(), P(), P())
    return jax.shard_map(local, mesh=split, in_specs=placed,
                         out_specs=(P(DP_OUTER, None), P(DP_OUTER, None), P()), check_vma=False)
```

```python
import functools, math
import jax, jax.numpy as jnp
from jax import lax
from jax.experimental import pallas as pl
from jax.experimental.pallas import tpu as pltpu
from jax.sharding import Mesh
from jax.sharding import PartitionSpec as P

DP_OUTER = ("dp_0", "dp_1", "dp_2", "outer")

STEPS = 1280
sigma_floor = 0.002
sigma_ceiling = 80.0
sigma_data = 0.5
huber_scale = 0.00054
rho_power = 7.0
F32, BF16 = jnp.float32, jnp.bfloat16
LAT, PATCHES, D, H, BUCKETS = 8, 112, 1024, 1024, 16
ROWS = LAT * PATCHES
TILE = (8, 128)
TN = 256
MB = 448
CORE, FIRST_AT, SECOND_AT = 0, 1, 2
VMEM = pl.BlockSpec(memory_space=pltpu.VMEM)
SMEM = pl.BlockSpec(memory_space=pltpu.SMEM)
ANY = pl.BlockSpec(memory_space=pltpu.HBM)


def rows_from(values):
    row = lax.broadcasted_iota(jnp.int32, TILE, 0)
    out = jnp.full(TILE, values[0])
    for k in range(1, len(values)):
        out = jnp.where(row == k, values[k], out)
    return out


def plan(index):
    ramp = index.astype(F32) / (STEPS - 1)
    top = sigma_ceiling ** (1.0 / rho_power)
    bottom = sigma_floor ** (1.0 / rho_power)
    base = top + ramp * (bottom - top)
    square = base * base
    fourth = square * square
    return fourth * square * base


def scale_factors(s):
    skip = sigma_data**2 / ((s - sigma_floor) ** 2 + sigma_data**2)
    scale = jnp.sqrt(s * s + sigma_data**2)
    return skip, (s - sigma_floor) * sigma_data / scale, 1.0 / scale


def sigmoid(x):
    return 0.5 * jnp.tanh(0.5 * x) + 0.5


def transposed_dot(a, b):
    return lax.dot_general(a, b, (((0,), (0,)), ((), ())), preferred_element_type=F32)


def store_routed(block, y, t, color, ref):
    v = block.reshape(32, 8, 256)
    left, right = v[:, :, :128], v[:, :, 128:]
    halves = (
        jnp.concatenate([left[:, :4], right[:, :4]], axis=1),
        jnp.concatenate([left[:, 4:], right[:, 4:]], axis=1),
    )
    for x in range(4):
        pieces = halves[x % 2].reshape(8, 2, 2, 8, 128)[:, :, x // 2]
        place = jnp.where(color == 0, x * 4 + y, y * 4 + x)
        for c in range(2):
            ref[pl.ds((place * 2 + t) * 16 + c * 8, 8)] = pieces[:, c]


def weight_gradient(left, right, right_cols, color, ref):
    def part(y, _):
        block = transposed_dot(left[:, pl.ds(pl.multiple_of(y * 256, 256), 256)], right[:, right_cols])
        for t in range(2):
            store_routed(block[:, t * TN:(t + 1) * TN], y, t, color, ref)
        return 0

    lax.fori_loop(0, 4, part, 0, unroll=True)


def half(color):
    return pl.ds(pl.multiple_of(color * 512, 512), 512)


def forward_kernel(place_hbm, t_index_hbm, bucket_id_hbm, bucket_count_hbm, clean_hbm, noise_hbm, w1, w2, t1, t2,
                   send, bucket, grad_out, pre_hi, inputs, act_hi,
                   clean, noise, in_lo, act_lo, diff, coef, wbuf, place, t_index, bucket_id, bucket_count,
                   field_sems, sems, small_sems, *, total):
    small = [pltpu.make_async_copy(src, dst, small_sems.at[k]) for k, (src, dst) in enumerate((
        (place_hbm, place), (t_index_hbm, t_index), (bucket_id_hbm, bucket_id), (bucket_count_hbm, bucket_count)))]
    fields = []
    for lat in range(LAT):
        rows = pl.ds(lat * PATCHES, PATCHES)
        fields.append((pltpu.make_async_copy(clean_hbm.at[lat], clean.at[rows], field_sems.at[0, lat]),
                       pltpu.make_async_copy(noise_hbm.at[lat], noise.at[rows], field_sems.at[1, lat])))
    copies = [pltpu.make_async_copy(src, wbuf.at[k], sems.at[k]) for k, src in enumerate((w1, t1, w2, t2))]
    for copy in small:
        copy.start()
    for pair in fields:
        pair[0].start()
        pair[1].start()
    for copy in copies:
        copy.start()
    for copy in small:
        copy.wait()
    hi_index = rows_from([t_index[k] for k in range(LAT)])
    s_hi, s_lo = plan(hi_index), plan(hi_index + 1)
    skip_hi, out_hi, in_scale_hi = scale_factors(s_hi)
    skip_lo, out_lo, in_scale_lo = scale_factors(s_lo)
    coef[0] = in_scale_hi
    coef[1] = in_scale_lo
    coef[2] = s_hi
    coef[3] = s_lo
    coef[4] = out_hi
    coef[5] = out_lo
    coef[6] = skip_hi
    coef[7] = skip_lo

    def one(k, lat):
        return coef[k, lat:lat + 1, 0:1]

    def block_rows(lat):
        return slice(lat * PATCHES, (lat + 1) * PATCHES)

    def field(lat, side, ref):
        rows = block_rows(lat)
        c, n = clean[rows, :].astype(F32), noise[rows, :].astype(F32)
        ref[rows, :] = (one(side, lat) * (c + one(2 + side, lat) * n)).astype(BF16)

    for lat in range(LAT):
        fields[lat][0].wait()
        fields[lat][1].wait()
        field(lat, 0, inputs)
        field(lat, 1, in_lo)
    copies[0].wait()
    for j in range(H // TN):
        cols = slice(j * TN, (j + 1) * TN)
        pre = jnp.dot(inputs[...], wbuf[0, :, cols], preferred_element_type=F32)
        act_hi[:, cols] = (pre * sigmoid(pre)).astype(BF16)
        pre_hi[:, cols] = pre
    copies[1].wait()
    for j in range(H // TN):
        cols = slice(j * TN, (j + 1) * TN)
        pre = jnp.dot(in_lo[...], wbuf[1, :, cols], preferred_element_type=F32)
        act_lo[:, cols] = (pre * sigmoid(pre)).astype(BF16)
    copies[2].wait()
    copies[3].wait()
    row = lax.broadcasted_iota(jnp.int32, TILE, 0)
    sums = jnp.zeros(TILE, F32)
    for j in range(D // TN):
        cols = slice(j * TN, (j + 1) * TN)
        for m in range(2):
            rows = slice(m * MB, (m + 1) * MB)
            online = jnp.dot(act_hi[rows, :], wbuf[2, :, cols], preferred_element_type=F32)
            target = jnp.dot(act_lo[rows, :], wbuf[3, :, cols], preferred_element_type=F32)
            for k in range(MB // PATCHES):
                lat = m * (MB // PATCHES) + k
                r, s = block_rows(lat), block_rows(k)
                c, n = clean[r, cols].astype(F32), noise[r, cols].astype(F32)
                on = one(6, lat) * (c + one(2, lat) * n) + one(4, lat) * online[s]
                tg = one(7, lat) * (c + one(3, lat) * n) + one(5, lat) * target[s]
                d = on - tg
                diff[r, cols] = d
                sq = jnp.sum((d * d).reshape(PATCHES // 8, 8, TN), axis=0)
                sq = sq[:, :128] + sq[:, 128:]
                sums = sums + jnp.where(row == lat, jnp.sum(sq, axis=0, keepdims=True), 0.0)
    q = jnp.sum(sums, axis=1, keepdims=True)
    c2 = huber_scale * math.sqrt(PATCHES * D)
    root = jnp.sqrt(q + c2**2)
    distance = root - c2
    count = rows_from([bucket_count[bucket_id[k]].astype(F32) for k in range(LAT)])
    weight = s_lo / (s_hi - s_lo) / jnp.sqrt(count) / total
    lane = lax.broadcasted_iota(jnp.int32, TILE, 1)
    part = jnp.where(lane == rows_from([bucket_id[k] for k in range(LAT)]), weight * distance, 0.0)
    bucket[...] = part
    send[512] = part
    coef[8] = out_hi * (weight / root)
    for lat in range(LAT):
        rows = block_rows(lat)
        grad_out[rows, :] = (one(8, lat) * diff[rows, :]).astype(BF16)
    color = 1 - place[CORE]
    weight_gradient(act_hi, grad_out, half(color), color, send)


def second_kernel(info, act_hi, grad_out, keep):
    weight_gradient(act_hi, grad_out, half(info[CORE]), info[CORE], keep)


def first_kernel(info, grad_out, pre_hi, inputs, w2, out, grad_pre, *, color_flip):
    color = 1 - info[CORE] if color_flip else info[CORE]
    cols = half(color)

    def back(m, _):
        rows = pl.ds(pl.multiple_of(m * 224, 224), 224)
        product = lax.dot_general(grad_out[rows, :], w2[cols, :], (((1,), (1,)), ((), ())), preferred_element_type=F32)
        pre = pre_hi[rows, cols]
        sig = sigmoid(pre)
        grad_pre[rows, :] = (product * (sig * (1.0 + pre * (1.0 - sig)))).astype(BF16)
        return 0

    lax.fori_loop(0, 4, back, 0, unroll=True)
    weight_gradient(inputs, grad_pre, slice(None), color, out)


def tiles(n):
    return jax.ShapeDtypeStruct((n, 8, 128), F32)


PRODUCT = 2 * ROWS * D * H


def forward(info, t_index, bucket_id, bucket_count, clean, noise, w1, w2, t1, t2, total):
    return pl.pallas_call(
        functools.partial(forward_kernel, total=total),
        out_shape=(pltpu.VMEM((513, 8, 128), F32), pltpu.VMEM(TILE, F32), pltpu.VMEM((ROWS, D), BF16),
                   pltpu.VMEM((ROWS, H), F32), pltpu.VMEM((ROWS, D), BF16), pltpu.VMEM((ROWS, H), BF16)),
        in_specs=[ANY] * 10,
        out_specs=(VMEM,) * 6,
        scratch_shapes=[pltpu.VMEM((ROWS, D), BF16), pltpu.VMEM((ROWS, D), BF16), pltpu.VMEM((ROWS, D), BF16),
                        pltpu.VMEM((ROWS, H), BF16), pltpu.VMEM((ROWS, D), F32), pltpu.VMEM((9,) + TILE, F32),
                        pltpu.VMEM((4, D, H), BF16), pltpu.SMEM((3,), jnp.int32), pltpu.SMEM((LAT,), jnp.int32),
                        pltpu.SMEM((LAT,), jnp.int32), pltpu.SMEM((BUCKETS,), jnp.int32),
                        pltpu.SemaphoreType.DMA((2, LAT)), pltpu.SemaphoreType.DMA((4,)), pltpu.SemaphoreType.DMA((4,))],
        compiler_params=pltpu.CompilerParams(vmem_limit_bytes=51 * 2**20),
        cost_estimate=pl.CostEstimate(flops=9 * PRODUCT // 2, bytes_accessed=24 * 2**20, transcendentals=2 * ROWS * H),
        name="forward",
    )(info, t_index, bucket_id, bucket_count, clean, noise, w1, w2, t1, t2)


def second_grad(info, act_hi, grad_out):
    return pl.pallas_call(
        second_kernel,
        out_shape=pltpu.VMEM((512, 8, 128), F32),
        in_specs=[SMEM, VMEM, VMEM],
        out_specs=VMEM,
        compiler_params=pltpu.CompilerParams(vmem_limit_bytes=16 * 2**20),
        cost_estimate=pl.CostEstimate(flops=PRODUCT // 2, bytes_accessed=4 * 2**20, transcendentals=0),
        name="second_grad",
    )(info, act_hi, grad_out)


def first_grad(info, grad_out, pre_hi, inputs, w2, color_flip, rows=pltpu.VMEM((512, 8, 128), F32)):
    return pl.pallas_call(
        functools.partial(first_kernel, color_flip=color_flip),
        out_shape=rows,
        in_specs=[SMEM] + [VMEM] * 4,
        out_specs=VMEM,
        scratch_shapes=[pltpu.VMEM((ROWS, 512), BF16)],
        compiler_params=pltpu.CompilerParams(vmem_limit_bytes=20 * 2**20),
        cost_estimate=pl.CostEstimate(flops=PRODUCT, bytes_accessed=8 * 2**20, transcendentals=0),
        name="first_grad",
    )(info, grad_out, pre_hi, inputs, w2)


def call(kernel, outs, ins, vmem_mib, flops, moved):
    return pl.pallas_call(
        kernel,
        out_shape=outs,
        in_specs=[SMEM] + [VMEM] * (len(ins) - 1),
        out_specs=tuple(VMEM for _ in outs),
        compiler_params=pltpu.CompilerParams(vmem_limit_bytes=vmem_mib * 2**20),
        cost_estimate=pl.CostEstimate(flops=flops, bytes_accessed=moved, transcendentals=0),
    )(*ins)


def core_sum_kernel(info, keep, came, *rest, with_bucket):
    bucket, (own, up, down, up_kept, down_kept) = (rest[0], rest[1:]) if with_bucket else (None, rest)

    def half(ref, at, ahead, t):
        p = (info[FIRST_AT] + ahead) % 4
        for q in range(4):
            src = pl.ds(pl.multiple_of(p * 128, 128) + q * 32 + t * 16, 16)
            ref[pl.ds(at + q * 16, 16)] = keep[src] + came[src]

    half(up, 0, 2, 0)
    half(up, 64, 1, 1)
    half(down, 0, 2, 1)
    half(down, 64, 3, 0)
    half(up_kept, 0, 1, 0)
    half(down_kept, 0, 3, 1)
    src = pl.ds(pl.multiple_of(info[FIRST_AT] * 128, 128), 128)
    own[pl.ds(0, 128)] = keep[src] + came[src]
    if with_bucket:
        both = bucket[...] + came[512]
        own[128] = both
        up[128] = both
        down[128] = both
        up_kept[64] = both


def core_sum(info, keep, came, bucket=None):
    more = 0 if bucket is None else 1
    outs = (tiles(128 + more),) * 3 + (tiles(64 + more), tiles(64))
    ins = (info, keep, came) if bucket is None else (info, keep, came, bucket)
    return call(functools.partial(core_sum_kernel, with_bucket=bucket is not None), outs, ins,
                10, 2**19, 6 * 2**20)


def middle_sum_kernel(info, came_up, came_down, up_kept, down_kept, up, down):
    up[pl.ds(0, 64)] = up_kept[pl.ds(0, 64)] + came_up[pl.ds(0, 64)]
    down[...] = down_kept[...] + came_down[pl.ds(0, 64)]
    if up.shape[0] > 64:
        up[64] = up_kept[64] + came_up[128]


def middle_sum(info, came_up, came_down, up_kept, down_kept):
    outs = (tiles(up_kept.shape[0]), tiles(64))
    return call(middle_sum_kernel, outs, (info, came_up, came_down, up_kept, down_kept),
                4, 2**17, 3 * 2**19)


def shift_pairs(k, x_on_core):
    pairs = []
    for y in range(4):
        for z in range(8):
            for core in range(2):
                for x in range(4):
                    to = (y, z, core, (x + k) % 4) if core == x_on_core else ((y + k) % 4, z, core, x)
                    pairs.append((((y * 8 + z) * 2 + core) * 4 + x, ((to[0] * 8 + to[1]) * 2 + to[2]) * 4 + to[3]))
    return pairs


def shift(piece, k, x_on_core):
    return lax.ppermute(piece, DP_OUTER, shift_pairs(k, x_on_core))


def around(info, own, up, down, up_kept, down_kept):
    came_up, came_down = shift(up, 1, 0), shift(down, 3, 0)
    up, down = middle_sum(info, came_up, came_down, up_kept, down_kept)
    up = shift(up, 1, 0)
    down = shift(down, 3, 0)
    return own, came_up, came_down, up, down


def plane_sum_kernel(info, *refs):
    second, first, pieces = refs[:5], refs[5:10], refs[10:]
    for k in range(4):
        q = (info[SECOND_AT] + k) % 4
        for g, (own, came_up, came_down, up, down) in enumerate((second, first)):
            here = pl.multiple_of(q * 32, 32)
            there = pl.multiple_of(q * 16, 16)
            pieces[k][pl.ds(g * 32, 16)] = own[pl.ds(here, 16)] + up[pl.ds(there, 16)] + came_down[pl.ds(64 + there, 16)]
            pieces[k][pl.ds(g * 32 + 16, 16)] = own[pl.ds(here + 16, 16)] + came_up[pl.ds(64 + there, 16)] + down[pl.ds(there, 16)]
        pieces[k][64] = second[0][128] + second[3][64] + second[2][128]


def plane_sum(info, second, first):
    return call(plane_sum_kernel, (tiles(65),) * 4, (info, *second, *first), 10, 2**20, 5 * 2**20)


def exchange(pieces, x_on_core):
    return [pieces[0]] + [shift(pieces[k], k, x_on_core) for k in (1, 3, 2)]


def line_sum_kernel(info, a, b, c, d, out):
    for g in range(2):
        for t in range(2):
            for core in range(2):
                at = pl.ds(g * 32 + t * 16 + core * 8, 8)
                out[:, core, 2 * g + t] = (a[at] + b[at]) + (c[at] + d[at])
    bucket = (a[64] + b[64]) + (c[64] + d[64])
    for z in range(8):
        for core in range(2):
            out[z, core, 4] = bucket


def line_sum(info, pieces):
    outs = (jax.ShapeDtypeStruct((8, 2, 5, 8, 128), F32),)
    return call(line_sum_kernel, outs, (info, *pieces), 4, 2**18, 2**20)[0]


def last_sum_kernel(info, came, first, second, bucket):
    def total(color, at):
        v = [came[2 * z + color, at] for z in range(8)]
        return ((v[0] + v[1]) + (v[2] + v[3])) + ((v[4] + v[5]) + (v[6] + v[7]))

    for g, ref in enumerate((second, first)):
        for color in range(2):
            for t in range(2):
                tile = total(color, 2 * g + t)
                at = (2 * color + t) * 256
                ref[:, at: at + 128] = tile[:4]
                ref[:, at + 128: at + 256] = tile[4:]
    bucket[...] = jnp.sum(total(0, 4), axis=0, keepdims=True)


def last_sum(info, came):
    outs = (jax.ShapeDtypeStruct((4, 1024), F32), jax.ShapeDtypeStruct((4, 1024), F32), jax.ShapeDtypeStruct((1, 128), F32))
    return call(last_sum_kernel, outs, (info, came), 2, 2**16, 2**19)


def other_core(array):
    return lax.ppermute(array, "dp_2", [(0, 1), (1, 0)])


def step(clean, noise, t_index, bucket_id, bucket_count, w_first, w_second, teacher_first, teacher_second):
    total = clean.shape[0] * lax.axis_size(DP_OUTER)
    core, x, y = lax.axis_index("dp_2"), lax.axis_index("outer"), lax.axis_index("dp_0")
    info = jnp.stack([core, jnp.where(core == 0, x, y), jnp.where(core == 0, y, x)]).astype(jnp.int32)
    send_s, bucket, grad_out, pre_hi, inputs, act_hi = forward(
        info, t_index, bucket_id, bucket_count, clean, noise, w_first, w_second, teacher_first, teacher_second, total)
    came_s = other_core(send_s)
    keep_s = second_grad(info, act_hi, grad_out)
    send_f = first_grad(info, grad_out, pre_hi, inputs, w_second, True)
    came_f = other_core(send_f)
    second = around(info, *core_sum(info, keep_s, came_s, bucket))
    keep_f = first_grad(info, grad_out, pre_hi, inputs, w_second, False)
    first = around(info, *core_sum(info, keep_f, came_f))
    pieces = exchange(plane_sum(info, second, first), 1)
    came = lax.all_to_all(line_sum(info, pieces).reshape(16, 5, 8, 128), ("dp_1", "dp_2"), 0, 0, tiled=True)
    first_rows, second_rows, losses = last_sum(info, came)
    return first_rows, second_rows, losses[0, :BUCKETS]


def solution(mesh):
    split = Mesh(mesh.devices.reshape(4, 8, 2, mesh.shape["outer"]), DP_OUTER)
    placed = (P(DP_OUTER, None, None), P(DP_OUTER, None, None), P(DP_OUTER), P(DP_OUTER), P(), P(), P(), P(), P())
    return jax.shard_map(step, mesh=split, in_specs=placed,
                         out_specs=(P(DP_OUTER, None), P(DP_OUTER, None), P()), check_vma=False)
```

```python
import functools, math
import jax, jax.numpy as jnp
from jax import lax
from jax.experimental import pallas as pl
from jax.experimental.pallas import tpu as pltpu
from jax.sharding import Mesh
from jax.sharding import PartitionSpec as P

DP_OUTER = ("dp_0", "dp_1", "dp_2", "outer")

STEPS = 1280
sigma_floor = 0.002
sigma_ceiling = 80.0
sigma_data = 0.5
huber_scale = 0.00054
rho_power = 7.0
F32, BF16 = jnp.float32, jnp.bfloat16
LAT, PATCHES, D, H, BUCKETS = 8, 112, 1024, 1024, 16
ROWS = LAT * PATCHES
TILE = (8, 128)
TN = 256
MB = 448
VMEM = pl.BlockSpec(memory_space=pltpu.VMEM)
ANY = pl.BlockSpec(memory_space=pltpu.HBM)


def core_index():
    return lax.axis_index("dp_2")


def along(first, ahead):
    on_x = core_index() == (0 if first else 1)
    return (jnp.where(on_x, lax.axis_index("outer"), lax.axis_index("dp_0")) + ahead) % 4


def rows_from(values):
    row = lax.broadcasted_iota(jnp.int32, TILE, 0)
    out = jnp.full(TILE, values[0])
    for k in range(1, len(values)):
        out = jnp.where(row == k, values[k], out)
    return out


def plan(index):
    ramp = index.astype(F32) / (STEPS - 1)
    top = sigma_ceiling ** (1.0 / rho_power)
    bottom = sigma_floor ** (1.0 / rho_power)
    base = top + ramp * (bottom - top)
    square = base * base
    fourth = square * square
    return fourth * square * base


def scale_factors(s):
    skip = sigma_data**2 / ((s - sigma_floor) ** 2 + sigma_data**2)
    scale = jnp.sqrt(s * s + sigma_data**2)
    return skip, (s - sigma_floor) * sigma_data / scale, 1.0 / scale


def sigmoid(x):
    return 0.5 * jnp.tanh(0.5 * x) + 0.5


def transposed_dot(a, b):
    return lax.dot_general(a, b, (((0,), (0,)), ((), ())), preferred_element_type=F32)


def store_routed(block, y, t, color, ref):
    v = block.reshape(32, 8, 256)
    left, right = v[:, :, :128], v[:, :, 128:]
    halves = (
        jnp.concatenate([left[:, :4], right[:, :4]], axis=1),
        jnp.concatenate([left[:, 4:], right[:, 4:]], axis=1),
    )
    for x in range(4):
        pieces = halves[x % 2].reshape(8, 2, 2, 8, 128)[:, :, x // 2]
        place = jnp.where(color == 0, x * 4 + y, y * 4 + x)
        for c in range(2):
            ref[pl.ds((place * 2 + t) * 16 + c * 8, 8)] = pieces[:, c]


def weight_gradient(left, right, right_cols, color, ref):
    def part(y, _):
        block = transposed_dot(left[:, pl.ds(pl.multiple_of(y * 256, 256), 256)], right[:, right_cols])
        for t in range(2):
            store_routed(block[:, t * TN:(t + 1) * TN], y, t, color, ref)
        return 0

    lax.fori_loop(0, 4, part, 0, unroll=True)


def half(color):
    return pl.ds(pl.multiple_of(color * 512, 512), 512)


def forward_kernel(t_index_hbm, bucket_id_hbm, bucket_count_hbm, clean_hbm, noise_hbm, w1, w2, t1, t2,
                   send, bucket, grad_out, pre_hi, inputs, act_hi,
                   clean, noise, in_lo, act_lo, diff, coef, wbuf, t_index, bucket_id, bucket_count,
                   field_sems, sems, small_sems, *, total):
    small = [pltpu.make_async_copy(src, dst, small_sems.at[k]) for k, (src, dst) in enumerate((
        (t_index_hbm, t_index), (bucket_id_hbm, bucket_id), (bucket_count_hbm, bucket_count)))]
    fields = []
    for lat in range(LAT):
        rows = pl.ds(lat * PATCHES, PATCHES)
        fields.append((pltpu.make_async_copy(clean_hbm.at[lat], clean.at[rows], field_sems.at[0, lat]),
                       pltpu.make_async_copy(noise_hbm.at[lat], noise.at[rows], field_sems.at[1, lat])))
    copies = [pltpu.make_async_copy(src, wbuf.at[k], sems.at[k]) for k, src in enumerate((w1, t1, w2, t2))]
    for copy in small:
        copy.start()
    for pair in fields:
        pair[0].start()
        pair[1].start()
    for copy in copies:
        copy.start()
    for copy in small:
        copy.wait()
    hi_index = rows_from([t_index[k] for k in range(LAT)])
    s_hi, s_lo = plan(hi_index), plan(hi_index + 1)
    skip_hi, out_hi, in_scale_hi = scale_factors(s_hi)
    skip_lo, out_lo, in_scale_lo = scale_factors(s_lo)
    coef[0] = in_scale_hi
    coef[1] = in_scale_lo
    coef[2] = s_hi
    coef[3] = s_lo
    coef[4] = out_hi
    coef[5] = out_lo
    coef[6] = skip_hi
    coef[7] = skip_lo

    def one(k, lat):
        return coef[k, lat:lat + 1, 0:1]

    def block_rows(lat):
        return slice(lat * PATCHES, (lat + 1) * PATCHES)

    def field(lat, side, ref):
        rows = block_rows(lat)
        c, n = clean[rows, :].astype(F32), noise[rows, :].astype(F32)
        ref[rows, :] = (one(side, lat) * (c + one(2 + side, lat) * n)).astype(BF16)

    for lat in range(LAT):
        fields[lat][0].wait()
        fields[lat][1].wait()
        field(lat, 0, inputs)
        field(lat, 1, in_lo)
    copies[0].wait()
    for j in range(H // TN):
        cols = slice(j * TN, (j + 1) * TN)
        pre = jnp.dot(inputs[...], wbuf[0, :, cols], preferred_element_type=F32)
        act_hi[:, cols] = (pre * sigmoid(pre)).astype(BF16)
        pre_hi[:, cols] = pre
    copies[1].wait()
    for j in range(H // TN):
        cols = slice(j * TN, (j + 1) * TN)
        pre = jnp.dot(in_lo[...], wbuf[1, :, cols], preferred_element_type=F32)
        act_lo[:, cols] = (pre * sigmoid(pre)).astype(BF16)
    copies[2].wait()
    copies[3].wait()
    row = lax.broadcasted_iota(jnp.int32, TILE, 0)
    sums = jnp.zeros(TILE, F32)
    for j in range(D // TN):
        cols = slice(j * TN, (j + 1) * TN)
        for m in range(2):
            rows = slice(m * MB, (m + 1) * MB)
            online = jnp.dot(act_hi[rows, :], wbuf[2, :, cols], preferred_element_type=F32)
            target = jnp.dot(act_lo[rows, :], wbuf[3, :, cols], preferred_element_type=F32)
            for k in range(MB // PATCHES):
                lat = m * (MB // PATCHES) + k
                r, s = block_rows(lat), block_rows(k)
                c, n = clean[r, cols].astype(F32), noise[r, cols].astype(F32)
                on = one(6, lat) * (c + one(2, lat) * n) + one(4, lat) * online[s]
                tg = one(7, lat) * (c + one(3, lat) * n) + one(5, lat) * target[s]
                d = on - tg
                diff[r, cols] = d
                sq = jnp.sum((d * d).reshape(PATCHES // 8, 8, TN), axis=0)
                sq = sq[:, :128] + sq[:, 128:]
                sums = sums + jnp.where(row == lat, jnp.sum(sq, axis=0, keepdims=True), 0.0)
    q = jnp.sum(sums, axis=1, keepdims=True)
    c2 = huber_scale * math.sqrt(PATCHES * D)
    root = jnp.sqrt(q + c2**2)
    distance = root - c2
    count = rows_from([bucket_count[bucket_id[k]].astype(F32) for k in range(LAT)])
    weight = s_lo / (s_hi - s_lo) / jnp.sqrt(count) / total
    lane = lax.broadcasted_iota(jnp.int32, TILE, 1)
    part = jnp.where(lane == rows_from([bucket_id[k] for k in range(LAT)]), weight * distance, 0.0)
    bucket[...] = part
    send[512] = part
    coef[8] = out_hi * (weight / root)
    for lat in range(LAT):
        rows = block_rows(lat)
        grad_out[rows, :] = (one(8, lat) * diff[rows, :]).astype(BF16)
    color = 1 - core_index()
    weight_gradient(act_hi, grad_out, half(color), color, send)


def second_kernel(act_hi, grad_out, keep):
    weight_gradient(act_hi, grad_out, half(core_index()), core_index(), keep)


def first_kernel(grad_out, pre_hi, inputs, w2, out, grad_pre, *, color_flip):
    color = 1 - core_index() if color_flip else core_index()
    cols = half(color)

    def back(m, _):
        rows = pl.ds(pl.multiple_of(m * 224, 224), 224)
        product = lax.dot_general(grad_out[rows, :], w2[cols, :], (((1,), (1,)), ((), ())), preferred_element_type=F32)
        pre = pre_hi[rows, cols]
        sig = sigmoid(pre)
        grad_pre[rows, :] = (product * (sig * (1.0 + pre * (1.0 - sig)))).astype(BF16)
        return 0

    lax.fori_loop(0, 4, back, 0, unroll=True)
    weight_gradient(inputs, grad_pre, slice(None), color, out)


def tiles(n):
    return jax.ShapeDtypeStruct((n, 8, 128), F32)


PRODUCT = 2 * ROWS * D * H


def forward(t_index, bucket_id, bucket_count, clean, noise, w1, w2, t1, t2, total):
    return pl.pallas_call(
        functools.partial(forward_kernel, total=total),
        out_shape=(pltpu.VMEM((513, 8, 128), F32), pltpu.VMEM(TILE, F32), pltpu.VMEM((ROWS, D), BF16),
                   pltpu.VMEM((ROWS, H), F32), pltpu.VMEM((ROWS, D), BF16), pltpu.VMEM((ROWS, H), BF16)),
        in_specs=[ANY] * 9,
        out_specs=(VMEM,) * 6,
        scratch_shapes=[pltpu.VMEM((ROWS, D), BF16), pltpu.VMEM((ROWS, D), BF16), pltpu.VMEM((ROWS, D), BF16),
                        pltpu.VMEM((ROWS, H), BF16), pltpu.VMEM((ROWS, D), F32), pltpu.VMEM((9,) + TILE, F32),
                        pltpu.VMEM((4, D, H), BF16), pltpu.SMEM((LAT,), jnp.int32),
                        pltpu.SMEM((LAT,), jnp.int32), pltpu.SMEM((BUCKETS,), jnp.int32),
                        pltpu.SemaphoreType.DMA((2, LAT)), pltpu.SemaphoreType.DMA((4,)), pltpu.SemaphoreType.DMA((3,))],
        compiler_params=pltpu.CompilerParams(vmem_limit_bytes=51 * 2**20),
        cost_estimate=pl.CostEstimate(flops=9 * PRODUCT // 2, bytes_accessed=24 * 2**20, transcendentals=2 * ROWS * H),
        name="forward",
    )(t_index, bucket_id, bucket_count, clean, noise, w1, w2, t1, t2)


def second_grad(act_hi, grad_out):
    return pl.pallas_call(
        second_kernel,
        out_shape=pltpu.VMEM((512, 8, 128), F32),
        in_specs=[VMEM, VMEM],
        out_specs=VMEM,
        compiler_params=pltpu.CompilerParams(vmem_limit_bytes=16 * 2**20),
        cost_estimate=pl.CostEstimate(flops=PRODUCT // 2, bytes_accessed=4 * 2**20, transcendentals=0),
        name="second_grad",
    )(act_hi, grad_out)


def first_grad(grad_out, pre_hi, inputs, w2, color_flip, rows=pltpu.VMEM((512, 8, 128), F32)):
    return pl.pallas_call(
        functools.partial(first_kernel, color_flip=color_flip),
        out_shape=rows,
        in_specs=[VMEM] * 4,
        out_specs=VMEM,
        scratch_shapes=[pltpu.VMEM((ROWS, 512), BF16)],
        compiler_params=pltpu.CompilerParams(vmem_limit_bytes=20 * 2**20),
        cost_estimate=pl.CostEstimate(flops=PRODUCT, bytes_accessed=8 * 2**20, transcendentals=0),
        name="first_grad",
    )(grad_out, pre_hi, inputs, w2)


def call(kernel, outs, ins, vmem_mib, flops, moved):
    return pl.pallas_call(
        kernel,
        out_shape=outs,
        in_specs=[VMEM] * len(ins),
        out_specs=tuple(VMEM for _ in outs),
        compiler_params=pltpu.CompilerParams(vmem_limit_bytes=vmem_mib * 2**20),
        cost_estimate=pl.CostEstimate(flops=flops, bytes_accessed=moved, transcendentals=0),
    )(*ins)


def core_sum_kernel(keep, came, *rest, with_bucket):
    bucket, (own, up, down, up_kept, down_kept) = (rest[0], rest[1:]) if with_bucket else (None, rest)

    def half(ref, at, ahead, t):
        p = along(True, ahead)
        for q in range(4):
            src = pl.ds(pl.multiple_of(p * 128, 128) + q * 32 + t * 16, 16)
            ref[pl.ds(at + q * 16, 16)] = keep[src] + came[src]

    half(up, 0, 2, 0)
    half(up, 64, 1, 1)
    half(down, 0, 2, 1)
    half(down, 64, 3, 0)
    half(up_kept, 0, 1, 0)
    half(down_kept, 0, 3, 1)
    src = pl.ds(pl.multiple_of(along(True, 0) * 128, 128), 128)
    own[pl.ds(0, 128)] = keep[src] + came[src]
    if with_bucket:
        both = bucket[...] + came[512]
        own[128] = both
        up[128] = both
        down[128] = both
        up_kept[64] = both


def core_sum(keep, came, bucket=None):
    more = 0 if bucket is None else 1
    outs = (tiles(128 + more),) * 3 + (tiles(64 + more), tiles(64))
    ins = (keep, came) if bucket is None else (keep, came, bucket)
    return call(functools.partial(core_sum_kernel, with_bucket=bucket is not None), outs, ins,
                10, 2**19, 6 * 2**20)


def middle_sum_kernel(came, kept, out):
    out[pl.ds(0, 64)] = kept[pl.ds(0, 64)] + came[pl.ds(0, 64)]
    if out.shape[0] > 64:
        out[64] = kept[64] + came[128]


def middle_sum(came, kept):
    return call(middle_sum_kernel, (tiles(kept.shape[0]),), (came, kept), 3, 2**16, 3 * 2**18)[0]


def shift_pairs(k, x_on_core):
    pairs = []
    for y in range(4):
        for z in range(8):
            for core in range(2):
                for x in range(4):
                    to = (y, z, core, (x + k) % 4) if core == x_on_core else ((y + k) % 4, z, core, x)
                    pairs.append((((y * 8 + z) * 2 + core) * 4 + x, ((to[0] * 8 + to[1]) * 2 + to[2]) * 4 + to[3]))
    return pairs


def shift(piece, k, x_on_core):
    return lax.ppermute(piece, DP_OUTER, shift_pairs(k, x_on_core))


def around(own, up, down, up_kept, down_kept):
    came_up, came_down = shift(up, 1, 0), shift(down, 3, 0)
    up = middle_sum(came_up, up_kept)
    up = shift(up, 1, 0)
    down = middle_sum(came_down, down_kept)
    down = shift(down, 3, 0)
    return own, came_up, came_down, up, down


def plane_sum_kernel(*refs):
    second, first, pieces = refs[:5], refs[5:10], refs[10:]
    for k in range(4):
        q = along(False, k)
        for g, (own, came_up, came_down, up, down) in enumerate((second, first)):
            here = pl.multiple_of(q * 32, 32)
            there = pl.multiple_of(q * 16, 16)
            pieces[k][pl.ds(g * 32, 16)] = own[pl.ds(here, 16)] + up[pl.ds(there, 16)] + came_down[pl.ds(64 + there, 16)]
            pieces[k][pl.ds(g * 32 + 16, 16)] = own[pl.ds(here + 16, 16)] + came_up[pl.ds(64 + there, 16)] + down[pl.ds(there, 16)]
        pieces[k][64] = second[0][128] + second[3][64] + second[2][128]


def plane_sum(second, first):
    return call(plane_sum_kernel, (tiles(65),) * 4, (*second, *first), 10, 2**20, 5 * 2**20)


def exchange(pieces, x_on_core):
    return [pieces[0]] + [shift(pieces[k], k, x_on_core) for k in (1, 3, 2)]


def line_sum_kernel(a, b, c, d, out):
    for g in range(2):
        for t in range(2):
            for core in range(2):
                at = pl.ds(g * 32 + t * 16 + core * 8, 8)
                out[:, core, 2 * g + t] = (a[at] + b[at]) + (c[at] + d[at])
    bucket = (a[64] + b[64]) + (c[64] + d[64])
    for z in range(8):
        for core in range(2):
            out[z, core, 4] = bucket


def line_sum(pieces):
    outs = (jax.ShapeDtypeStruct((8, 2, 5, 8, 128), F32),)
    return call(line_sum_kernel, outs, tuple(pieces), 4, 2**18, 2**20)[0]


def last_sum_kernel(came, first, second, bucket):
    def total(color, at):
        v = [came[2 * z + color, at] for z in range(8)]
        return ((v[0] + v[1]) + (v[2] + v[3])) + ((v[4] + v[5]) + (v[6] + v[7]))

    for g, ref in enumerate((second, first)):
        for color in range(2):
            for t in range(2):
                tile = total(color, 2 * g + t)
                at = (2 * color + t) * 256
                ref[:, at: at + 128] = tile[:4]
                ref[:, at + 128: at + 256] = tile[4:]
    bucket[...] = jnp.sum(total(0, 4), axis=0, keepdims=True)[:, :BUCKETS]


def last_sum(came):
    outs = (jax.ShapeDtypeStruct((4, 1024), F32), jax.ShapeDtypeStruct((4, 1024), F32), jax.ShapeDtypeStruct((1, BUCKETS), F32))
    return call(last_sum_kernel, outs, (came,), 2, 2**16, 2**19)


def other_core(array):
    return lax.ppermute(array, "dp_2", [(0, 1), (1, 0)])


def step(clean, noise, t_index, bucket_id, bucket_count, w_first, w_second, teacher_first, teacher_second):
    total = clean.shape[0] * lax.axis_size(DP_OUTER)
    send_s, bucket, grad_out, pre_hi, inputs, act_hi = forward(
        t_index, bucket_id, bucket_count, clean, noise, w_first, w_second, teacher_first, teacher_second, total)
    came_s = other_core(send_s)
    keep_s = second_grad(act_hi, grad_out)
    send_f = first_grad(grad_out, pre_hi, inputs, w_second, True)
    came_f = other_core(send_f)
    second = around(*core_sum(keep_s, came_s, bucket))
    keep_f = first_grad(grad_out, pre_hi, inputs, w_second, False)
    first = around(*core_sum(keep_f, came_f))
    pieces = exchange(plane_sum(second, first), 1)
    came = lax.all_to_all(line_sum(pieces).reshape(16, 5, 8, 128), ("dp_1", "dp_2"), 0, 0, tiled=True)
    first_rows, second_rows, losses = last_sum(came)
    return first_rows, second_rows, losses.reshape(BUCKETS)


def solution(mesh):
    split = Mesh(mesh.devices.reshape(4, 8, 2, mesh.shape["outer"]), DP_OUTER)
    placed = (P(DP_OUTER, None, None), P(DP_OUTER, None, None), P(DP_OUTER), P(DP_OUTER), P(), P(), P(), P(), P())
    return jax.shard_map(step, mesh=split, in_specs=placed,
                         out_specs=(P(DP_OUTER, None), P(DP_OUTER, None), P()), check_vma=False)
```

```python
import functools, math
import jax, jax.numpy as jnp
from jax import lax
from jax.experimental import pallas as pl
from jax.experimental.pallas import tpu as pltpu
from jax.sharding import Mesh
from jax.sharding import PartitionSpec as P

DP_OUTER = ("dp_0", "dp_1", "dp_2", "outer")

STEPS = 1280
sigma_floor = 0.002
sigma_ceiling = 80.0
sigma_data = 0.5
huber_scale = 0.00054
rho_power = 7.0
F32, BF16 = jnp.float32, jnp.bfloat16
LAT, PATCHES, D, H, BUCKETS = 8, 112, 1024, 1024, 16
ROWS = LAT * PATCHES
TILE = (8, 128)
TN = 256
MB = 448
VMEM = pl.BlockSpec(memory_space=pltpu.VMEM)
ANY = pl.BlockSpec(memory_space=pltpu.HBM)


def core_index():
    return lax.axis_index("dp_2")


def along(first, ahead):
    on_x = core_index() == (0 if first else 1)
    return (jnp.where(on_x, lax.axis_index("outer"), lax.axis_index("dp_0")) + ahead) % 4


def rows_from(values):
    row = lax.broadcasted_iota(jnp.int32, TILE, 0)
    out = jnp.full(TILE, values[0])
    for k in range(1, len(values)):
        out = jnp.where(row == k, values[k], out)
    return out


def plan(index):
    ramp = index.astype(F32) / (STEPS - 1)
    top = sigma_ceiling ** (1.0 / rho_power)
    bottom = sigma_floor ** (1.0 / rho_power)
    base = top + ramp * (bottom - top)
    square = base * base
    fourth = square * square
    return fourth * square * base


def scale_factors(s):
    skip = sigma_data**2 / ((s - sigma_floor) ** 2 + sigma_data**2)
    scale = jnp.sqrt(s * s + sigma_data**2)
    return skip, (s - sigma_floor) * sigma_data / scale, 1.0 / scale


def sigmoid(x):
    return 0.5 * jnp.tanh(0.5 * x) + 0.5


def transposed_dot(a, b):
    return lax.dot_general(a, b, (((0,), (0,)), ((), ())), preferred_element_type=F32)


def store_routed(block, y, t, color, ref):
    v = block.reshape(32, 8, 256)
    left, right = v[:, :, :128], v[:, :, 128:]
    halves = (
        jnp.concatenate([left[:, :4], right[:, :4]], axis=1),
        jnp.concatenate([left[:, 4:], right[:, 4:]], axis=1),
    )
    for x in range(4):
        pieces = halves[x % 2].reshape(8, 2, 2, 8, 128)[:, :, x // 2]
        place = jnp.where(color == 0, x * 4 + y, y * 4 + x)
        for c in range(2):
            ref[pl.ds((place * 2 + t) * 16 + c * 8, 8)] = pieces[:, c]


def weight_gradient(left, right, right_cols, color, ref):
    def part(y, _):
        block = transposed_dot(left[:, pl.ds(pl.multiple_of(y * 256, 256), 256)], right[:, right_cols])
        for t in range(2):
            store_routed(block[:, t * TN:(t + 1) * TN], y, t, color, ref)
        return 0

    lax.fori_loop(0, 4, part, 0, unroll=True)


def half(color):
    return pl.ds(pl.multiple_of(color * 512, 512), 512)


def forward_kernel(t_index_hbm, bucket_id_hbm, bucket_count_hbm, clean_hbm, noise_hbm, w1, w2, t1, t2,
                   send, bucket, grad_out, pre_hi, inputs, act_hi,
                   clean, noise, in_lo, act_lo, diff, coef, wbuf, t_index, bucket_id, bucket_count,
                   field_sems, sems, small_sems, *, total):
    small = [pltpu.make_async_copy(src, dst, small_sems.at[k]) for k, (src, dst) in enumerate((
        (t_index_hbm, t_index), (bucket_id_hbm, bucket_id), (bucket_count_hbm, bucket_count)))]
    fields = []
    for lat in range(LAT):
        rows = pl.ds(lat * PATCHES, PATCHES)
        fields.append((pltpu.make_async_copy(clean_hbm.at[lat], clean.at[rows], field_sems.at[0, lat]),
                       pltpu.make_async_copy(noise_hbm.at[lat], noise.at[rows], field_sems.at[1, lat])))
    copies = [pltpu.make_async_copy(src, wbuf.at[k], sems.at[k]) for k, src in enumerate((w1, t1, w2, t2))]
    for copy in small:
        copy.start()
    for pair in fields:
        pair[0].start()
        pair[1].start()
    for copy in copies:
        copy.start()
    for copy in small:
        copy.wait()
    hi_index = rows_from([t_index[k] for k in range(LAT)])
    s_hi, s_lo = plan(hi_index), plan(hi_index + 1)
    skip_hi, out_hi, in_scale_hi = scale_factors(s_hi)
    skip_lo, out_lo, in_scale_lo = scale_factors(s_lo)
    coef[0] = in_scale_hi
    coef[1] = in_scale_lo
    coef[2] = s_hi
    coef[3] = s_lo
    coef[4] = out_hi
    coef[5] = out_lo
    coef[6] = skip_hi
    coef[7] = skip_lo

    def one(k, lat):
        return coef[k, lat:lat + 1, 0:1]

    def block_rows(lat):
        return slice(lat * PATCHES, (lat + 1) * PATCHES)

    def field(lat, side, ref):
        rows = block_rows(lat)
        c, n = clean[rows, :].astype(F32), noise[rows, :].astype(F32)
        ref[rows, :] = (one(side, lat) * (c + one(2 + side, lat) * n)).astype(BF16)

    for lat in range(LAT):
        fields[lat][0].wait()
        fields[lat][1].wait()
        field(lat, 0, inputs)
        field(lat, 1, in_lo)
    copies[0].wait()
    for j in range(H // TN):
        cols = slice(j * TN, (j + 1) * TN)
        pre = jnp.dot(inputs[...], wbuf[0, :, cols], preferred_element_type=F32)
        act_hi[:, cols] = (pre * sigmoid(pre)).astype(BF16)
        pre_hi[:, cols] = pre
    copies[1].wait()
    for j in range(H // TN):
        cols = slice(j * TN, (j + 1) * TN)
        pre = jnp.dot(in_lo[...], wbuf[1, :, cols], preferred_element_type=F32)
        act_lo[:, cols] = (pre * sigmoid(pre)).astype(BF16)
    copies[2].wait()
    copies[3].wait()
    row = lax.broadcasted_iota(jnp.int32, TILE, 0)
    sums = jnp.zeros(TILE, F32)
    for j in range(D // TN):
        cols = slice(j * TN, (j + 1) * TN)
        for m in range(2):
            rows = slice(m * MB, (m + 1) * MB)
            online = jnp.dot(act_hi[rows, :], wbuf[2, :, cols], preferred_element_type=F32)
            target = jnp.dot(act_lo[rows, :], wbuf[3, :, cols], preferred_element_type=F32)
            for k in range(MB // PATCHES):
                lat = m * (MB // PATCHES) + k
                r, s = block_rows(lat), block_rows(k)
                c, n = clean[r, cols].astype(F32), noise[r, cols].astype(F32)
                on = one(6, lat) * (c + one(2, lat) * n) + one(4, lat) * online[s]
                tg = one(7, lat) * (c + one(3, lat) * n) + one(5, lat) * target[s]
                d = on - tg
                diff[r, cols] = d
                sq = jnp.sum((d * d).reshape(PATCHES // 8, 8, TN), axis=0)
                sq = sq[:, :128] + sq[:, 128:]
                sums = sums + jnp.where(row == lat, jnp.sum(sq, axis=0, keepdims=True), 0.0)
    q = jnp.sum(sums, axis=1, keepdims=True)
    c2 = huber_scale * math.sqrt(PATCHES * D)
    root = jnp.sqrt(q + c2**2)
    distance = root - c2
    count = rows_from([bucket_count[bucket_id[k]].astype(F32) for k in range(LAT)])
    weight = s_lo / (s_hi - s_lo) / jnp.sqrt(count) / total
    lane = lax.broadcasted_iota(jnp.int32, TILE, 1)
    part = jnp.where(lane == rows_from([bucket_id[k] for k in range(LAT)]), weight * distance, 0.0)
    bucket[...] = part
    send[512] = part
    coef[8] = out_hi * (weight / root)
    for lat in range(LAT):
        rows = block_rows(lat)
        grad_out[rows, :] = (one(8, lat) * diff[rows, :]).astype(BF16)
    color = 1 - core_index()
    weight_gradient(act_hi, grad_out, half(color), color, send)


def second_kernel(act_hi, grad_out, keep):
    weight_gradient(act_hi, grad_out, half(core_index()), core_index(), keep)


def first_kernel(grad_out, pre_hi, inputs, w2, out, grad_pre, *, color_flip):
    color = 1 - core_index() if color_flip else core_index()
    cols = half(color)

    def back(m, _):
        rows = pl.ds(pl.multiple_of(m * 224, 224), 224)
        product = lax.dot_general(grad_out[rows, :], w2[cols, :], (((1,), (1,)), ((), ())), preferred_element_type=F32)
        pre = pre_hi[rows, cols]
        sig = sigmoid(pre)
        grad_pre[rows, :] = (product * (sig * (1.0 + pre * (1.0 - sig)))).astype(BF16)
        return 0

    lax.fori_loop(0, 4, back, 0, unroll=True)
    weight_gradient(inputs, grad_pre, slice(None), color, out)


def tiles(n):
    return jax.ShapeDtypeStruct((n, 8, 128), F32)


PRODUCT = 2 * ROWS * D * H


def forward(t_index, bucket_id, bucket_count, clean, noise, w1, w2, t1, t2, total):
    return pl.pallas_call(
        functools.partial(forward_kernel, total=total),
        out_shape=(pltpu.VMEM((513, 8, 128), F32), pltpu.VMEM(TILE, F32), pltpu.VMEM((ROWS, D), BF16),
                   pltpu.VMEM((ROWS, H), F32), pltpu.VMEM((ROWS, D), BF16), pltpu.VMEM((ROWS, H), BF16)),
        in_specs=[ANY] * 9,
        out_specs=(VMEM,) * 6,
        scratch_shapes=[pltpu.VMEM((ROWS, D), BF16), pltpu.VMEM((ROWS, D), BF16), pltpu.VMEM((ROWS, D), BF16),
                        pltpu.VMEM((ROWS, H), BF16), pltpu.VMEM((ROWS, D), F32), pltpu.VMEM((9,) + TILE, F32),
                        pltpu.VMEM((4, D, H), BF16), pltpu.SMEM((LAT,), jnp.int32),
                        pltpu.SMEM((LAT,), jnp.int32), pltpu.SMEM((BUCKETS,), jnp.int32),
                        pltpu.SemaphoreType.DMA((2, LAT)), pltpu.SemaphoreType.DMA((4,)), pltpu.SemaphoreType.DMA((3,))],
        compiler_params=pltpu.CompilerParams(vmem_limit_bytes=51 * 2**20),
        cost_estimate=pl.CostEstimate(flops=9 * PRODUCT // 2, bytes_accessed=24 * 2**20, transcendentals=2 * ROWS * H),
        name="forward",
    )(t_index, bucket_id, bucket_count, clean, noise, w1, w2, t1, t2)


def second_grad(act_hi, grad_out):
    return pl.pallas_call(
        second_kernel,
        out_shape=pltpu.VMEM((512, 8, 128), F32),
        in_specs=[VMEM, VMEM],
        out_specs=VMEM,
        compiler_params=pltpu.CompilerParams(vmem_limit_bytes=16 * 2**20),
        cost_estimate=pl.CostEstimate(flops=PRODUCT // 2, bytes_accessed=4 * 2**20, transcendentals=0),
        name="second_grad",
    )(act_hi, grad_out)


def first_grad(grad_out, pre_hi, inputs, w2, color_flip, rows=pltpu.VMEM((512, 8, 128), F32)):
    return pl.pallas_call(
        functools.partial(first_kernel, color_flip=color_flip),
        out_shape=rows,
        in_specs=[VMEM] * 4,
        out_specs=VMEM,
        scratch_shapes=[pltpu.VMEM((ROWS, 512), BF16)],
        compiler_params=pltpu.CompilerParams(vmem_limit_bytes=20 * 2**20),
        cost_estimate=pl.CostEstimate(flops=PRODUCT, bytes_accessed=8 * 2**20, transcendentals=0),
        name="first_grad",
    )(grad_out, pre_hi, inputs, w2)


def call(kernel, outs, ins, vmem_mib, flops, moved):
    return pl.pallas_call(
        kernel,
        out_shape=outs,
        in_specs=[VMEM] * len(ins),
        out_specs=tuple(VMEM for _ in outs),
        compiler_params=pltpu.CompilerParams(vmem_limit_bytes=vmem_mib * 2**20),
        cost_estimate=pl.CostEstimate(flops=flops, bytes_accessed=moved, transcendentals=0),
    )(*ins)


def core_sum_kernel(keep, came, *rest, with_bucket):
    bucket, (own, up, down, up_kept, down_kept) = (rest[0], rest[1:]) if with_bucket else (None, rest)

    def half(ref, at, ahead, t):
        p = along(True, ahead)
        for q in range(4):
            src = pl.ds(pl.multiple_of(p * 128, 128) + q * 32 + t * 16, 16)
            ref[pl.ds(at + q * 16, 16)] = keep[src] + came[src]

    half(up, 0, 2, 0)
    half(up, 64, 1, 1)
    half(down, 0, 2, 1)
    half(down, 64, 3, 0)
    half(up_kept, 0, 1, 0)
    half(down_kept, 0, 3, 1)
    src = pl.ds(pl.multiple_of(along(True, 0) * 128, 128), 128)
    own[pl.ds(0, 128)] = keep[src] + came[src]
    if with_bucket:
        both = bucket[...] + came[512]
        own[128] = both
        up[128] = both
        down[128] = both
        up_kept[64] = both


def core_sum(keep, came, bucket=None):
    more = 0 if bucket is None else 1
    outs = (tiles(128 + more),) * 3 + (tiles(64 + more), tiles(64))
    ins = (keep, came) if bucket is None else (keep, came, bucket)
    return call(functools.partial(core_sum_kernel, with_bucket=bucket is not None), outs, ins,
                10, 2**19, 6 * 2**20)


def middle_sum_kernel(came, kept, out):
    out[pl.ds(0, 64)] = kept[pl.ds(0, 64)] + came[pl.ds(0, 64)]
    if out.shape[0] > 64:
        out[64] = kept[64] + came[128]


def middle_sum(came, kept):
    return call(middle_sum_kernel, (tiles(kept.shape[0]),), (came, kept), 3, 2**16, 3 * 2**18)[0]


def shift_pairs(k, x_on_core):
    pairs = []
    for y in range(4):
        for z in range(8):
            for core in range(2):
                for x in range(4):
                    to = (y, z, core, (x + k) % 4) if core == x_on_core else ((y + k) % 4, z, core, x)
                    pairs.append((((y * 8 + z) * 2 + core) * 4 + x, ((to[0] * 8 + to[1]) * 2 + to[2]) * 4 + to[3]))
    return pairs


def shift(piece, k, x_on_core):
    return lax.ppermute(piece, DP_OUTER, shift_pairs(k, x_on_core))


def around(own, up, down, up_kept, down_kept):
    came_up, came_down = shift(up, 1, 0), shift(down, 3, 0)
    up = middle_sum(came_up, up_kept)
    up = shift(up, 1, 0)
    down = middle_sum(came_down, down_kept)
    down = shift(down, 3, 0)
    return own, came_up, came_down, up, down


def plane_sum_kernel(own, came_up, came_down, up, down, *pieces):
    for k in range(4):
        q = along(False, k)
        here = pl.multiple_of(q * 32, 32)
        there = pl.multiple_of(q * 16, 16)
        pieces[k][pl.ds(0, 16)] = own[pl.ds(here, 16)] + up[pl.ds(there, 16)] + came_down[pl.ds(64 + there, 16)]
        pieces[k][pl.ds(16, 16)] = own[pl.ds(here + 16, 16)] + came_up[pl.ds(64 + there, 16)] + down[pl.ds(there, 16)]
        if own.shape[0] > 128:
            pieces[k][32] = own[128] + up[64] + came_down[128]


def plane_sum(ins):
    return call(plane_sum_kernel, (tiles(ins[0].shape[0] - 96),) * 4, tuple(ins), 6, 2**19, 5 * 2**19)


def exchange(pieces, x_on_core):
    came = [pieces[0]]
    for k in (1, 3, 2):
        came.append(shift(pieces[k], k, x_on_core))
    return came


def line_sum_kernel(*refs):
    second, first, out = refs[:4], refs[4:8], refs[8]
    for g, (a, b, c, d) in enumerate((second, first)):
        for t in range(2):
            for core in range(2):
                at = pl.ds(t * 16 + core * 8, 8)
                out[:, core, 2 * g + t] = (a[at] + b[at]) + (c[at] + d[at])
    bucket = (second[0][32] + second[1][32]) + (second[2][32] + second[3][32])
    for z in range(8):
        for core in range(2):
            out[z, core, 4] = bucket


def line_sum(second, first):
    outs = (jax.ShapeDtypeStruct((8, 2, 5, 8, 128), F32),)
    return call(line_sum_kernel, outs, (*second, *first), 4, 2**18, 2**20)[0]


def last_sum_kernel(came, first, second, bucket):
    def total(color, at):
        v = [came[2 * z + color, at] for z in range(8)]
        return ((v[0] + v[1]) + (v[2] + v[3])) + ((v[4] + v[5]) + (v[6] + v[7]))

    for g, ref in enumerate((second, first)):
        for color in range(2):
            for t in range(2):
                tile = total(color, 2 * g + t)
                at = (2 * color + t) * 256
                ref[:, at: at + 128] = tile[:4]
                ref[:, at + 128: at + 256] = tile[4:]
    bucket[...] = jnp.sum(total(0, 4), axis=0, keepdims=True)[:, :BUCKETS]


def last_sum(came):
    outs = (jax.ShapeDtypeStruct((4, 1024), F32), jax.ShapeDtypeStruct((4, 1024), F32), jax.ShapeDtypeStruct((1, BUCKETS), F32))
    return call(last_sum_kernel, outs, (came,), 2, 2**16, 2**19)


def other_core(array):
    return lax.ppermute(array, "dp_2", [(0, 1), (1, 0)])


def step(clean, noise, t_index, bucket_id, bucket_count, w_first, w_second, teacher_first, teacher_second):
    total = clean.shape[0] * lax.axis_size(DP_OUTER)
    send_s, bucket, grad_out, pre_hi, inputs, act_hi = forward(
        t_index, bucket_id, bucket_count, clean, noise, w_first, w_second, teacher_first, teacher_second, total)
    came_s = other_core(send_s)
    keep_s = second_grad(act_hi, grad_out)
    send_f = first_grad(grad_out, pre_hi, inputs, w_second, True)
    came_f = other_core(send_f)
    second = around(*core_sum(keep_s, came_s, bucket))
    keep_f = first_grad(grad_out, pre_hi, inputs, w_second, False)
    first = around(*core_sum(keep_f, came_f))
    second = exchange(plane_sum(second), 1)
    first = exchange(plane_sum(first), 1)
    came = lax.all_to_all(line_sum(second, first).reshape(16, 5, 8, 128), ("dp_1", "dp_2"), 0, 0, tiled=True)
    first_rows, second_rows, losses = last_sum(came)
    return first_rows, second_rows, losses.reshape(BUCKETS)


def solution(mesh):
    split = Mesh(mesh.devices.reshape(4, 8, 2, mesh.shape["outer"]), DP_OUTER)
    placed = (P(DP_OUTER, None, None), P(DP_OUTER, None, None), P(DP_OUTER), P(DP_OUTER), P(), P(), P(), P(), P())
    return jax.shard_map(step, mesh=split, in_specs=placed,
                         out_specs=(P(DP_OUTER, None), P(DP_OUTER, None), P()), check_vma=False)
```

```python
import functools, math
import jax, jax.numpy as jnp
from jax import lax
from jax.experimental import pallas as pl
from jax.experimental.pallas import tpu as pltpu
from jax.sharding import Mesh
from jax.sharding import PartitionSpec as P

DP_OUTER = ("dp_0", "dp_1", "dp_2", "outer")

STEPS = 1280
sigma_floor = 0.002
sigma_ceiling = 80.0
sigma_data = 0.5
huber_scale = 0.00054
rho_power = 7.0
F32, BF16 = jnp.float32, jnp.bfloat16
LAT, PATCHES, D, H, BUCKETS = 8, 112, 1024, 1024, 16
ROWS = LAT * PATCHES
TILE = (8, 128)
TN = 256
MB = 448
VMEM = pl.BlockSpec(memory_space=pltpu.VMEM)
ANY = pl.BlockSpec(memory_space=pltpu.HBM)


def core_index():
    return lax.axis_index("dp_2")


def along(first, ahead):
    on_x = core_index() == (0 if first else 1)
    return (jnp.where(on_x, lax.axis_index("outer"), lax.axis_index("dp_0")) + ahead) % 4


def rows_from(values):
    row = lax.broadcasted_iota(jnp.int32, TILE, 0)
    out = jnp.full(TILE, values[0])
    for k in range(1, len(values)):
        out = jnp.where(row == k, values[k], out)
    return out


def plan(index):
    ramp = index.astype(F32) / (STEPS - 1)
    top = sigma_ceiling ** (1.0 / rho_power)
    bottom = sigma_floor ** (1.0 / rho_power)
    base = top + ramp * (bottom - top)
    square = base * base
    fourth = square * square
    return fourth * square * base


def scale_factors(s):
    skip = sigma_data**2 / ((s - sigma_floor) ** 2 + sigma_data**2)
    scale = jnp.sqrt(s * s + sigma_data**2)
    return skip, (s - sigma_floor) * sigma_data / scale, 1.0 / scale


def sigmoid(x):
    return 0.5 * jnp.tanh(0.5 * x) + 0.5


def transposed_dot(a, b):
    return lax.dot_general(a, b, (((0,), (0,)), ((), ())), preferred_element_type=F32)


def store_routed(block, y, t, color, ref):
    v = block.reshape(32, 8, 256)
    left, right = v[:, :, :128], v[:, :, 128:]
    halves = (
        jnp.concatenate([left[:, :4], right[:, :4]], axis=1),
        jnp.concatenate([left[:, 4:], right[:, 4:]], axis=1),
    )
    for x in range(4):
        pieces = halves[x % 2].reshape(8, 2, 2, 8, 128)[:, :, x // 2]
        place = jnp.where(color == 0, x * 4 + y, y * 4 + x)
        for c in range(2):
            ref[pl.ds((place * 2 + t) * 16 + c * 8, 8)] = pieces[:, c]


def weight_gradient(left, right, right_cols, color, ref):
    def part(y, _):
        block = transposed_dot(left[:, pl.ds(pl.multiple_of(y * 256, 256), 256)], right[:, right_cols])
        for t in range(2):
            store_routed(block[:, t * TN:(t + 1) * TN], y, t, color, ref)
        return 0

    lax.fori_loop(0, 4, part, 0, unroll=True)


def half(color):
    return pl.ds(pl.multiple_of(color * 512, 512), 512)


def forward_kernel(t_index_hbm, bucket_id_hbm, bucket_count_hbm, clean_hbm, noise_hbm, w1, w2, t1, t2,
                   send, bucket, grad_out, pre_hi, inputs, act_hi,
                   clean, noise, in_lo, act_lo, diff, coef, wbuf, t_index, bucket_id, bucket_count,
                   field_sems, sems, small_sems, *, total):
    small = [pltpu.make_async_copy(src, dst, small_sems.at[k]) for k, (src, dst) in enumerate((
        (t_index_hbm, t_index), (bucket_id_hbm, bucket_id), (bucket_count_hbm, bucket_count)))]
    fields = []
    for lat in range(LAT):
        rows = pl.ds(lat * PATCHES, PATCHES)
        fields.append((pltpu.make_async_copy(clean_hbm.at[lat], clean.at[rows], field_sems.at[0, lat]),
                       pltpu.make_async_copy(noise_hbm.at[lat], noise.at[rows], field_sems.at[1, lat])))
    copies = [pltpu.make_async_copy(src, wbuf.at[k], sems.at[k]) for k, src in enumerate((w1, t1, w2, t2))]
    for copy in small:
        copy.start()
    for pair in fields:
        pair[0].start()
        pair[1].start()
    for copy in copies:
        copy.start()
    for copy in small:
        copy.wait()
    hi_index = rows_from([t_index[k] for k in range(LAT)])
    s_hi, s_lo = plan(hi_index), plan(hi_index + 1)
    skip_hi, out_hi, in_scale_hi = scale_factors(s_hi)
    skip_lo, out_lo, in_scale_lo = scale_factors(s_lo)
    coef[0] = in_scale_hi
    coef[1] = in_scale_lo
    coef[2] = s_hi
    coef[3] = s_lo
    coef[4] = out_hi
    coef[5] = out_lo
    coef[6] = skip_hi
    coef[7] = skip_lo

    def one(k, lat):
        return coef[k, lat:lat + 1, 0:1]

    def block_rows(lat):
        return slice(lat * PATCHES, (lat + 1) * PATCHES)

    def field(lat, side, ref):
        rows = block_rows(lat)
        c, n = clean[rows, :].astype(F32), noise[rows, :].astype(F32)
        ref[rows, :] = (one(side, lat) * (c + one(2 + side, lat) * n)).astype(BF16)

    for lat in range(LAT):
        fields[lat][0].wait()
        fields[lat][1].wait()
        field(lat, 0, inputs)
        field(lat, 1, in_lo)
    copies[0].wait()
    for j in range(H // TN):
        cols = slice(j * TN, (j + 1) * TN)
        pre = jnp.dot(inputs[...], wbuf[0, :, cols], preferred_element_type=F32)
        act_hi[:, cols] = (pre * sigmoid(pre)).astype(BF16)
        pre_hi[:, cols] = pre
    copies[1].wait()
    for j in range(H // TN):
        cols = slice(j * TN, (j + 1) * TN)
        pre = jnp.dot(in_lo[...], wbuf[1, :, cols], preferred_element_type=F32)
        act_lo[:, cols] = (pre * sigmoid(pre)).astype(BF16)
    copies[2].wait()
    copies[3].wait()
    row = lax.broadcasted_iota(jnp.int32, TILE, 0)
    sums = jnp.zeros(TILE, F32)
    for j in range(D // TN):
        cols = slice(j * TN, (j + 1) * TN)
        for m in range(2):
            rows = slice(m * MB, (m + 1) * MB)
            online = jnp.dot(act_hi[rows, :], wbuf[2, :, cols], preferred_element_type=F32)
            target = jnp.dot(act_lo[rows, :], wbuf[3, :, cols], preferred_element_type=F32)
            for k in range(MB // PATCHES):
                lat = m * (MB // PATCHES) + k
                r, s = block_rows(lat), block_rows(k)
                c, n = clean[r, cols].astype(F32), noise[r, cols].astype(F32)
                on = one(6, lat) * (c + one(2, lat) * n) + one(4, lat) * online[s]
                tg = one(7, lat) * (c + one(3, lat) * n) + one(5, lat) * target[s]
                d = on - tg
                diff[r, cols] = d
                sq = jnp.sum((d * d).reshape(PATCHES // 8, 8, TN), axis=0)
                sq = sq[:, :128] + sq[:, 128:]
                sums = sums + jnp.where(row == lat, jnp.sum(sq, axis=0, keepdims=True), 0.0)
    q = jnp.sum(sums, axis=1, keepdims=True)
    c2 = huber_scale * math.sqrt(PATCHES * D)
    root = jnp.sqrt(q + c2**2)
    distance = root - c2
    count = rows_from([bucket_count[bucket_id[k]].astype(F32) for k in range(LAT)])
    weight = s_lo / (s_hi - s_lo) / jnp.sqrt(count) / total
    lane = lax.broadcasted_iota(jnp.int32, TILE, 1)
    part = jnp.where(lane == rows_from([bucket_id[k] for k in range(LAT)]), weight * distance, 0.0)
    bucket[...] = part
    send[512] = part
    coef[8] = out_hi * (weight / root)
    for lat in range(LAT):
        rows = block_rows(lat)
        grad_out[rows, :] = (one(8, lat) * diff[rows, :]).astype(BF16)
    color = 1 - core_index()
    weight_gradient(act_hi, grad_out, half(color), color, send)


def second_kernel(act_hi, grad_out, keep):
    weight_gradient(act_hi, grad_out, half(core_index()), core_index(), keep)


def first_kernel(grad_out, pre_hi, inputs, w2, out, grad_pre, *, color_flip):
    color = 1 - core_index() if color_flip else core_index()
    cols = half(color)

    def back(m, _):
        rows = pl.ds(pl.multiple_of(m * 224, 224), 224)
        product = lax.dot_general(grad_out[rows, :], w2[cols, :], (((1,), (1,)), ((), ())), preferred_element_type=F32)
        pre = pre_hi[rows, cols]
        sig = sigmoid(pre)
        grad_pre[rows, :] = (product * (sig * (1.0 + pre * (1.0 - sig)))).astype(BF16)
        return 0

    lax.fori_loop(0, 4, back, 0, unroll=True)
    weight_gradient(inputs, grad_pre, slice(None), color, out)


def tiles(n):
    return jax.ShapeDtypeStruct((n, 8, 128), F32)


PRODUCT = 2 * ROWS * D * H


def forward(t_index, bucket_id, bucket_count, clean, noise, w1, w2, t1, t2, total):
    return pl.pallas_call(
        functools.partial(forward_kernel, total=total),
        out_shape=(pltpu.VMEM((513, 8, 128), F32), pltpu.VMEM(TILE, F32), pltpu.VMEM((ROWS, D), BF16),
                   pltpu.VMEM((ROWS, H), F32), pltpu.VMEM((ROWS, D), BF16), pltpu.VMEM((ROWS, H), BF16)),
        in_specs=[ANY] * 9,
        out_specs=(VMEM,) * 6,
        scratch_shapes=[pltpu.VMEM((ROWS, D), BF16), pltpu.VMEM((ROWS, D), BF16), pltpu.VMEM((ROWS, D), BF16),
                        pltpu.VMEM((ROWS, H), BF16), pltpu.VMEM((ROWS, D), F32), pltpu.VMEM((9,) + TILE, F32),
                        pltpu.VMEM((4, D, H), BF16), pltpu.SMEM((LAT,), jnp.int32),
                        pltpu.SMEM((LAT,), jnp.int32), pltpu.SMEM((BUCKETS,), jnp.int32),
                        pltpu.SemaphoreType.DMA((2, LAT)), pltpu.SemaphoreType.DMA((4,)), pltpu.SemaphoreType.DMA((3,))],
        compiler_params=pltpu.CompilerParams(vmem_limit_bytes=51 * 2**20),
        cost_estimate=pl.CostEstimate(flops=9 * PRODUCT // 2, bytes_accessed=24 * 2**20, transcendentals=2 * ROWS * H),
        name="forward",
    )(t_index, bucket_id, bucket_count, clean, noise, w1, w2, t1, t2)


def second_grad(act_hi, grad_out):
    return pl.pallas_call(
        second_kernel,
        out_shape=pltpu.VMEM((512, 8, 128), F32),
        in_specs=[VMEM, VMEM],
        out_specs=VMEM,
        compiler_params=pltpu.CompilerParams(vmem_limit_bytes=16 * 2**20),
        cost_estimate=pl.CostEstimate(flops=PRODUCT // 2, bytes_accessed=4 * 2**20, transcendentals=0),
        name="second_grad",
    )(act_hi, grad_out)


def first_grad(grad_out, pre_hi, inputs, w2, color_flip, rows=pltpu.VMEM((512, 8, 128), F32)):
    return pl.pallas_call(
        functools.partial(first_kernel, color_flip=color_flip),
        out_shape=rows,
        in_specs=[VMEM] * 4,
        out_specs=VMEM,
        scratch_shapes=[pltpu.VMEM((ROWS, 512), BF16)],
        compiler_params=pltpu.CompilerParams(vmem_limit_bytes=20 * 2**20),
        cost_estimate=pl.CostEstimate(flops=PRODUCT, bytes_accessed=8 * 2**20, transcendentals=0),
        name="first_grad",
    )(grad_out, pre_hi, inputs, w2)


def call(kernel, outs, ins, vmem_mib, flops, moved):
    return pl.pallas_call(
        kernel,
        out_shape=outs,
        in_specs=[VMEM] * len(ins),
        out_specs=tuple(VMEM for _ in outs),
        compiler_params=pltpu.CompilerParams(vmem_limit_bytes=vmem_mib * 2**20),
        cost_estimate=pl.CostEstimate(flops=flops, bytes_accessed=moved, transcendentals=0),
    )(*ins)


def core_sum_kernel(keep, came, *rest, with_bucket):
    bucket, (own, up, down, up_kept, down_kept) = (rest[0], rest[1:]) if with_bucket else (None, rest)

    def half(ref, at, ahead, t):
        p = along(True, ahead)
        for q in range(4):
            src = pl.ds(pl.multiple_of(p * 128, 128) + q * 32 + t * 16, 16)
            ref[pl.ds(at + q * 16, 16)] = keep[src] + came[src]

    half(up, 0, 2, 0)
    half(up, 64, 1, 1)
    half(down, 0, 2, 1)
    half(down, 64, 3, 0)
    half(up_kept, 0, 1, 0)
    half(down_kept, 0, 3, 1)
    src = pl.ds(pl.multiple_of(along(True, 0) * 128, 128), 128)
    own[pl.ds(0, 128)] = keep[src] + came[src]
    if with_bucket:
        both = bucket[...] + came[512]
        own[128] = both
        up[128] = both
        down[128] = both
        up_kept[64] = both


def core_sum(keep, came, bucket=None):
    more = 0 if bucket is None else 1
    outs = (tiles(128 + more),) * 3 + (tiles(64 + more), tiles(64))
    ins = (keep, came) if bucket is None else (keep, came, bucket)
    return call(functools.partial(core_sum_kernel, with_bucket=bucket is not None), outs, ins,
                10, 2**19, 6 * 2**20)


def middle_sum_kernel(came, kept, out):
    out[pl.ds(0, 64)] = kept[pl.ds(0, 64)] + came[pl.ds(0, 64)]
    if out.shape[0] > 64:
        out[64] = kept[64] + came[128]


def middle_sum(came, kept):
    return call(middle_sum_kernel, (tiles(kept.shape[0]),), (came, kept), 3, 2**16, 3 * 2**18)[0]


def shift_pairs(k, x_on_core):
    pairs = []
    for y in range(4):
        for z in range(8):
            for core in range(2):
                for x in range(4):
                    to = (y, z, core, (x + k) % 4) if core == x_on_core else ((y + k) % 4, z, core, x)
                    pairs.append((((y * 8 + z) * 2 + core) * 4 + x, ((to[0] * 8 + to[1]) * 2 + to[2]) * 4 + to[3]))
    return pairs


def shift(piece, k, x_on_core):
    return lax.ppermute(piece, DP_OUTER, shift_pairs(k, x_on_core))


def around(own, up, down, up_kept, down_kept):
    came_up = shift(up, 1, 0)
    came_down = shift(down, 3, 0)
    up = middle_sum(came_up, up_kept)
    up = shift(up, 1, 0)
    down = middle_sum(came_down, down_kept)
    down = shift(down, 3, 0)
    return own, came_up, came_down, up, down


def plane_sum_kernel(*refs):
    second, first, pieces = refs[:5], refs[5:10], refs[10:]
    for k in range(4):
        q = along(False, k)
        for g, (own, came_up, came_down, up, down) in enumerate((second, first)):
            here = pl.multiple_of(q * 32, 32)
            there = pl.multiple_of(q * 16, 16)
            pieces[k][pl.ds(g * 32, 16)] = own[pl.ds(here, 16)] + up[pl.ds(there, 16)] + came_down[pl.ds(64 + there, 16)]
            pieces[k][pl.ds(g * 32 + 16, 16)] = own[pl.ds(here + 16, 16)] + came_up[pl.ds(64 + there, 16)] + down[pl.ds(there, 16)]
        pieces[k][64] = second[0][128] + second[3][64] + second[2][128]


def plane_sum(second, first):
    return call(plane_sum_kernel, (tiles(65),) * 4, (*second, *first), 10, 2**20, 5 * 2**20)


def exchange(pieces, x_on_core):
    return [pieces[0]] + [shift(pieces[k], k, x_on_core) for k in (2, 1, 3)]


def line_sum_kernel(a, b, c, d, out):
    for g in range(2):
        for t in range(2):
            for core in range(2):
                at = pl.ds(g * 32 + t * 16 + core * 8, 8)
                out[:, core, 2 * g + t] = (a[at] + b[at]) + (c[at] + d[at])
    bucket = (a[64] + b[64]) + (c[64] + d[64])
    for z in range(8):
        for core in range(2):
            out[z, core, 4] = bucket


def line_sum(pieces):
    outs = (jax.ShapeDtypeStruct((8, 2, 5, 8, 128), F32),)
    return call(line_sum_kernel, outs, tuple(pieces), 4, 2**18, 2**20)[0]


def last_sum_kernel(came, first, second, bucket):
    def total(color, at):
        v = [came[2 * z + color, at] for z in range(8)]
        return ((v[0] + v[1]) + (v[2] + v[3])) + ((v[4] + v[5]) + (v[6] + v[7]))

    for g, ref in enumerate((second, first)):
        for color in range(2):
            for t in range(2):
                tile = total(color, 2 * g + t)
                at = (2 * color + t) * 256
                ref[:, at: at + 128] = tile[:4]
                ref[:, at + 128: at + 256] = tile[4:]
    bucket[...] = jnp.sum(total(0, 4), axis=0, keepdims=True)[:, :BUCKETS]


def last_sum(came):
    outs = (jax.ShapeDtypeStruct((4, 1024), F32), jax.ShapeDtypeStruct((4, 1024), F32), jax.ShapeDtypeStruct((1, BUCKETS), F32))
    return call(last_sum_kernel, outs, (came,), 2, 2**16, 2**19)


def other_core(array):
    return lax.ppermute(array, "dp_2", [(0, 1), (1, 0)])


def step(clean, noise, t_index, bucket_id, bucket_count, w_first, w_second, teacher_first, teacher_second):
    total = clean.shape[0] * lax.axis_size(DP_OUTER)
    send_s, bucket, grad_out, pre_hi, inputs, act_hi = forward(
        t_index, bucket_id, bucket_count, clean, noise, w_first, w_second, teacher_first, teacher_second, total)
    came_s = other_core(send_s)
    keep_s = second_grad(act_hi, grad_out)
    send_f = first_grad(grad_out, pre_hi, inputs, w_second, True)
    came_f = other_core(send_f)
    second = around(*core_sum(keep_s, came_s, bucket))
    keep_f = first_grad(grad_out, pre_hi, inputs, w_second, False)
    first = around(*core_sum(keep_f, came_f))
    pieces = exchange(plane_sum(second, first), 1)
    came = lax.all_to_all(line_sum(pieces).reshape(16, 5, 8, 128), ("dp_1", "dp_2"), 0, 0, tiled=True)
    first_rows, second_rows, losses = last_sum(came)
    return first_rows, second_rows, losses.reshape(BUCKETS)


def solution(mesh):
    split = Mesh(mesh.devices.reshape(4, 8, 2, mesh.shape["outer"]), DP_OUTER)
    placed = (P(DP_OUTER, None, None), P(DP_OUTER, None, None), P(DP_OUTER), P(DP_OUTER), P(), P(), P(), P(), P())
    return jax.shard_map(step, mesh=split, in_specs=placed,
                         out_specs=(P(DP_OUTER, None), P(DP_OUTER, None), P()), check_vma=False)
```
